256 devices in a mesh: gx: 16 (over z, y_lo), gy: 16 (over x, y_hi, core).
Axes of the slice: x: 4, y: 4 (y_hi: 2, y_lo: 2; y = y_hi * 2 + y_lo), z: 8, core: 2. Of those that a mesh axis runs over, the one named last changes fastest.
Arguments:
- preserved_vector: float32 [14, 128, 128, 128], P(None, 'gx', 'gy'), may hold values from -200 to 200, as said below
- nasa_table: float32 [32, 6], replicated, may hold values from -4 to 4.5, as said below
- gas_constant: float32 [32], replicated, may hold values from 0.3 to 3
- species_index: int32 [9], replicated, may hold values from 0 to 31, as said below
- face_kind: int32 [16, 16, 2], P('gx', 'gy'), may hold values from 0 to 1
Outputs:
- increment: float32 [14, 128, 128, 128], P(None, 'gx', 'gy')
The draws below stay inside these ranges and needn't reach their ends.
Inputs may be any that keep to these rules, and one draw needn't show every extreme that they name: `preserved_vector`: every cell is a physical state: positive partial densities and an energy whose temperature lies between 0.5 and 2.5. `nasa_table`: each row's cp over R polynomial exceeds 1.5 for temperatures 0.3 to 3. `species_index`: 9 distinct rows.
All inputs are finite; a program needn't handle non-finite values.
Results may differ from the reference program's by a relative error of at most 0.0003.
Values sent between devices are 32-bit elements; how exact they have to be, the bound alone decides.
No kernel may reach another device: no remote copies, remote signals or barrier semaphores. Data moves between devices by JAX's collectives and lax.ppermute only.
A program may use at most 64 MiB of HBM per device.

```python
import math
import jax
import jax.numpy as jnp
from jax import lax

NS = 9
NVAR = 14
KINDS = 32
NEWTON = 2
CX = 8
CY = 8
NX = 128
NY = 128
NZ = 128
N_GX = 16
N_GY = 16


def thermo_tables(key):
    lower = jnp.array([2.5, 0.0, -0.05, -0.01, -0.002, -4.0], jnp.float32)
    upper = jnp.array([4.5, 0.6, 0.05, 0.01, 0.002, 4.0], jnp.float32)
    table = lower + (upper - lower) * jax.random.uniform(jax.random.fold_in(key, 101), (KINDS, 6), jnp.float32)
    gases = jnp.exp(jax.random.uniform(jax.random.fold_in(key, 102), (KINDS,), jnp.float32, math.log(0.3), math.log(3.0)))
    middle_rows = (jax.random.permutation(jax.random.fold_in(key, 103), KINDS - 2)[:NS - 2] + 1).astype(jnp.int32)
    end_rows = jnp.array([0, KINDS - 1], jnp.int32)
    pooled = jnp.concatenate([end_rows, middle_rows], axis=0)
    shuffle = jax.random.permutation(jax.random.fold_in(key, 104), NS).astype(jnp.int32)
    chosen = pooled[shuffle].astype(jnp.int32)
    return (table, gases, chosen)


def draw_nasa_table(key, part):
    return thermo_tables(key)[0]


def draw_gas_constant(key, part):
    return thermo_tables(key)[1]


def draw_species_index(key, part):
    return thermo_tables(key)[2]


def draw_preserved_vector(key, part):
    table, gases, chosen = thermo_tables(key)
    nasa_table_weights = table[chosen]
    component_kind_r_factor = gases[chosen]
    grid_sizes_list = (NX, NY, NZ)
    draw_seed_handles_list = [jax.random.fold_in(key, 200 + number) for number in range(6)]
    abscissa_place = (jnp.arange(NX, dtype=jnp.float32) / NX)[:, None, None]
    ordinate_place = (jnp.arange(NY, dtype=jnp.float32) / NY)[None, :, None]
    ramp = 0.3 + 1.35 * (abscissa_place + ordinate_place)
    bulk_compactness = jnp.exp(jax.random.uniform(draw_seed_handles_list[0], grid_sizes_list, jnp.float32, -0.4, 0.4))
    fractions = jax.nn.softmax(jax.random.normal(draw_seed_handles_list[1], (NS,) + grid_sizes_list, jnp.float32), axis=0)
    passive = jax.random.uniform(draw_seed_handles_list[2], grid_sizes_list, jnp.float32)
    kelvin_reading = jax.random.uniform(draw_seed_handles_list[3], grid_sizes_list, jnp.float32, 0.5, 2.4)
    velocity = 0.5 * ramp[None] * jnp.clip(jax.random.normal(draw_seed_handles_list[4], (3,) + grid_sizes_list, jnp.float32), -4.0, 4.0)
    prefix_addition_result = bulk_compactness[None] * fractions
    replicated_layer = kelvin_reading[None]
    columns = [nasa_table_weights[:, degree].reshape((NS, 1, 1, 1)) for degree in range(6)]
    chemical_heat_content = columns[5] + replicated_layer * (columns[0] + replicated_layer * (columns[1] / 2.0 + replicated_layer * (columns[2] / 3.0 + replicated_layer * (columns[3] / 4.0 + replicated_layer * columns[4] / 5.0))))
    caloric_tiers = component_kind_r_factor.reshape((NS, 1, 1, 1)) * (chemical_heat_content - replicated_layer)
    energy = jnp.sum(prefix_addition_result * caloric_tiers, axis=0) + 0.5 * bulk_compactness * jnp.sum(velocity * velocity, axis=0)
    return jnp.concatenate([prefix_addition_result, bulk_compactness[None] * velocity, energy[None], (bulk_compactness * passive)[None]], axis=0).astype(jnp.float32)


def set_ends(values, key, least, high):
    dims = values.shape
    index_at = [jax.random.randint(jax.random.fold_in(key, axis), (), 0, dims[axis]) for axis in range(len(dims))]
    values = values.at[tuple(index_at)].set(least)
    longest = dims.index(max(dims))
    index_at[longest] = (index_at[longest] + 1) % dims[longest]
    return values.at[tuple(index_at)].set(high)


def setup_inputs(seed: int = 0) -> dict:
    arg_keys = jax.random.split(jax.random.key(seed), 6)
    preserved_vector = draw_preserved_vector(jax.random.fold_in(arg_keys[5], 71), 0)
    nasa_table = draw_nasa_table(jax.random.fold_in(arg_keys[5], 71), 0)
    gas_constant = draw_gas_constant(jax.random.fold_in(arg_keys[5], 71), 0)
    species_index = draw_species_index(jax.random.fold_in(arg_keys[5], 71), 0)
    face_kind = set_ends(jax.random.randint(arg_keys[4], (N_GX, N_GY, 2), 0, 2), jax.random.fold_in(arg_keys[4], 1), 0, 1).astype(jnp.int32)
    return {"preserved_vector": preserved_vector, "nasa_table": nasa_table, "gas_constant": gas_constant, "species_index": species_index, "face_kind": face_kind}


EPSILON = 1e-06
COURANT = 0.8

def column(vector, trailing_sizes):
    return vector.reshape((vector.shape[0],) + (1,) * trailing_sizes)

def caloric_fitted_curves_table(nasa_table_weights, kelvin_reading):
    trailing_sizes = kelvin_reading.ndim
    columns = [column(nasa_table_weights[:, degree], trailing_sizes) for degree in range(6)]
    replicated_layer = kelvin_reading[None]
    caloric_quotient = columns[0] + replicated_layer * (columns[1] + replicated_layer * (columns[2] + replicated_layer * (columns[3] + replicated_layer * columns[4])))
    chemical_heat_content = columns[5] + replicated_layer * (columns[0] + replicated_layer * (columns[1] / 2.0 + replicated_layer * (columns[2] / 3.0 + replicated_layer * (columns[3] / 4.0 + replicated_layer * columns[4] / 5.0))))
    return (caloric_quotient, chemical_heat_content)

def solve_for_kelvin(preserved_vector_lines, nasa_table_weights, component_kind_r_factor):
    prefix_addition_result = preserved_vector_lines[:NS]
    bulk_compactness = lax.optimization_barrier(jnp.sum(prefix_addition_result, axis=0))
    momentum = preserved_vector_lines[NS:NS + 3]
    caloric_content_inner = preserved_vector_lines[NS + 3] - 0.5 * lax.optimization_barrier(jnp.sum(momentum * momentum, axis=0)) / bulk_compactness
    blend_stack_lane = column(component_kind_r_factor, bulk_compactness.ndim)
    kelvin_reading = jnp.ones_like(bulk_compactness)
    for iteration in range(NEWTON):
        caloric_quotient, chemical_heat_content = caloric_fitted_curves_table(nasa_table_weights, kelvin_reading)
        solver_misfit = lax.optimization_barrier(jnp.sum(prefix_addition_result * blend_stack_lane * (chemical_heat_content - kelvin_reading[None]), axis=0)) - caloric_content_inner
        tangent_steepness_fn = lax.optimization_barrier(jnp.sum(prefix_addition_result * blend_stack_lane * (caloric_quotient - 1.0), axis=0))
        kelvin_reading = kelvin_reading - solver_misfit / tangent_steepness_fn
    return kelvin_reading

def nasa_fitted_monomials(preserved_vector_lines, kelvin_reading, nasa_table_weights, component_kind_r_factor):
    prefix_addition_result = preserved_vector_lines[:NS]
    bulk_compactness = lax.optimization_barrier(jnp.sum(prefix_addition_result, axis=0))
    momentum = preserved_vector_lines[NS:NS + 3]
    doubled_norm_motion = lax.optimization_barrier(jnp.sum(momentum * momentum, axis=0)) / (bulk_compactness * bulk_compactness)
    blend_stack_lane = column(component_kind_r_factor, bulk_compactness.ndim)
    caloric_quotient, chemical_heat_content = caloric_fitted_curves_table(nasa_table_weights, kelvin_reading)
    caloric_tiers = blend_stack_lane * (chemical_heat_content - kelvin_reading[None])
    averaged_mixing_law_r = lax.optimization_barrier(jnp.sum(prefix_addition_result * blend_stack_lane, axis=0))
    thrust_load_quiet = averaged_mixing_law_r * kelvin_reading
    heat_quotient_decrement = averaged_mixing_law_r / lax.optimization_barrier(jnp.sum(prefix_addition_result * blend_stack_lane * (caloric_quotient - 1.0), axis=0))
    sound_speed = jnp.sqrt((1.0 + heat_quotient_decrement) * thrust_load_quiet / bulk_compactness)
    force_spatial_jump = blend_stack_lane * kelvin_reading[None] - heat_quotient_decrement[None] * caloric_tiers + 0.5 * heat_quotient_decrement[None] * doubled_norm_motion[None]
    return jnp.concatenate([thrust_load_quiet[None], heat_quotient_decrement[None], sound_speed[None], force_spatial_jump], axis=0)

def reconstruct(values):
    value_zero, value_one, value_two, value_three, value_four = values
    candidate_zero = (2.0 * value_zero - 7.0 * value_one + 11.0 * value_two) / 6.0
    candidate_one = (-value_one + 5.0 * value_two + 2.0 * value_three) / 6.0
    candidate_two = (2.0 * value_two + 5.0 * value_three - value_four) / 6.0
    curve_zero = value_zero - 2.0 * value_one + value_two
    slope_zero = value_zero - 4.0 * value_one + 3.0 * value_two
    curve_one = value_one - 2.0 * value_two + value_three
    slope_one = value_one - value_three
    curve_two = value_two - 2.0 * value_three + value_four
    slope_two = 3.0 * value_two - 4.0 * value_three + value_four
    smooth_zero = 13.0 / 12.0 * curve_zero * curve_zero + 0.25 * slope_zero * slope_zero
    smooth_one = 13.0 / 12.0 * curve_one * curve_one + 0.25 * slope_one * slope_one
    smooth_two = 13.0 / 12.0 * curve_two * curve_two + 0.25 * slope_two * slope_two
    weight_zero = 0.1 / ((EPSILON + smooth_zero) * (EPSILON + smooth_zero))
    weight_one = 0.6 / ((EPSILON + smooth_one) * (EPSILON + smooth_one))
    weight_two = 0.3 / ((EPSILON + smooth_two) * (EPSILON + smooth_two))
    return (weight_zero * candidate_zero + weight_one * candidate_one + weight_two * candidate_two) / (weight_zero + weight_one + weight_two)

def window(array, offset, count, array_axis):
    return lax.slice_in_dim(array, offset, offset + count, axis=array_axis)

def direction_rate(preserved_vector_lines, cell_coef, array_axis, normal, speed):
    cells = preserved_vector_lines.shape[array_axis] - 6
    faces = cells + 1
    bulk_compactness = lax.optimization_barrier(jnp.sum(preserved_vector_lines[:NS], axis=0))
    fractions = preserved_vector_lines[:NS] / bulk_compactness[None]
    velocity = preserved_vector_lines[NS:NS + 3] / bulk_compactness[None]
    passive = preserved_vector_lines[NS + 4:NS + 5] / bulk_compactness[None]
    thrust_load_quiet = cell_coef[0]
    normal_speed = velocity[normal]
    carried = preserved_vector_lines * normal_speed[None]
    flux_rows = [carried[:NS]]
    for component in range(3):
        if component == normal:
            flux_rows.append((carried[NS + component] + thrust_load_quiet)[None])
        else:
            flux_rows.append(carried[NS + component][None])
    flux_rows.append((carried[NS + 3] + thrust_load_quiet * normal_speed)[None])
    flux_rows.append(carried[NS + 4][None])
    physical = jnp.concatenate(flux_rows, axis=0)
    upwind = 0.5 * (physical + speed * preserved_vector_lines)
    downwind = 0.5 * (physical - speed * preserved_vector_lines)

    def average(array):
        return 0.5 * (window(array, 2, faces, array_axis) + window(array, 3, faces, array_axis))
    mean_frac = average(fractions)
    mean_vel = average(velocity)
    mean_passive = average(passive)[0]
    mean_gamma = average(cell_coef[1:2])[0]
    mean_sound = average(cell_coef[2:3])[0]
    mean_slopes = average(cell_coef[3:])
    mean_square = lax.optimization_barrier(jnp.sum(mean_vel * mean_vel, axis=0))
    mean_enthalpy = (mean_sound * mean_sound - lax.optimization_barrier(jnp.sum(mean_frac * mean_slopes, axis=0))) / mean_gamma + mean_square
    inverse = 1.0 / (mean_sound * mean_sound)
    tangents = [component for component in range(3) if component != normal]

    def project(vector):
        total = lax.optimization_barrier(jnp.sum(vector[:NS], axis=0))
        pressure_jump = lax.optimization_barrier(jnp.sum(mean_slopes * vector[:NS], axis=0)) - mean_gamma * lax.optimization_barrier(jnp.sum(mean_vel * vector[NS:NS + 3], axis=0)) + mean_gamma * vector[NS + 3]
        normal_jump = vector[NS + normal] - mean_vel[normal] * total
        scaled = pressure_jump * inverse
        slower = 0.5 * (pressure_jump - mean_sound * normal_jump) * inverse
        faster = 0.5 * (pressure_jump + mean_sound * normal_jump) * inverse
        species = vector[:NS] - mean_frac * scaled[None]
        first_shear = vector[NS + tangents[0]] - mean_vel[tangents[0]] * total
        second_shear = vector[NS + tangents[1]] - mean_vel[tangents[1]] * total
        scalar_wave = vector[NS + 4] - mean_passive * scaled
        return jnp.concatenate([slower[None], species, first_shear[None], second_shear[None], faster[None], scalar_wave[None]], axis=0)
    rising = reconstruct([project(window(upwind, offset, faces, array_axis)) for offset in (0, 1, 2, 3, 4)])
    falling = reconstruct([project(window(downwind, offset, faces, array_axis)) for offset in (5, 4, 3, 2, 1)])
    amplitude = rising + falling
    slower = amplitude[0]
    species = amplitude[1:NS + 1]
    first_shear = amplitude[NS + 1]
    second_shear = amplitude[NS + 2]
    faster = amplitude[NS + 3]
    scalar_wave = amplitude[NS + 4]
    species_total = lax.optimization_barrier(jnp.sum(species, axis=0))
    acoustic = slower + faster
    normal_vel = mean_vel[normal]
    momentum_rows = []
    for component in range(3):
        if component == normal:
            momentum_rows.append((normal_vel - mean_sound) * slower + (normal_vel + mean_sound) * faster + normal_vel * species_total)
        elif component == tangents[0]:
            momentum_rows.append(mean_vel[component] * (acoustic + species_total) + first_shear)
        else:
            momentum_rows.append(mean_vel[component] * (acoustic + species_total) + second_shear)
    energy_row = (mean_enthalpy - normal_vel * mean_sound) * slower + (mean_enthalpy + normal_vel * mean_sound) * faster + lax.optimization_barrier(jnp.sum((mean_square[None] - mean_slopes / mean_gamma[None]) * species, axis=0)) + mean_vel[tangents[0]] * first_shear + mean_vel[tangents[1]] * second_shear
    face_flux = jnp.concatenate([mean_frac * acoustic[None] + species, jnp.stack(momentum_rows, axis=0), energy_row[None], (mean_passive * acoustic + scalar_wave)[None]], axis=0)
    return window(face_flux, 0, cells, array_axis) - window(face_flux, 1, cells, array_axis)

def wall_pad(payload, lower_kind, upper_kind):
    rows_count = payload.shape[0]
    sign_flips = jnp.where(jnp.arange(rows_count) == NS + 2, -1.0, 1.0).astype(payload.dtype).reshape((rows_count, 1, 1, 1))
    lower_copy = jnp.concatenate([payload[..., :1]] * 3, axis=3)
    upper_copy = jnp.concatenate([payload[..., -1:]] * 3, axis=3)
    lower_mirror = payload[..., 2::-1] * sign_flips
    upper_mirror = payload[..., :-4:-1] * sign_flips
    lower_ghost = jnp.where(lower_kind == 1, lower_mirror, lower_copy)
    upper_ghost = jnp.where(upper_kind == 1, upper_mirror, upper_copy)
    return jnp.concatenate([lower_ghost, payload, upper_ghost], axis=3)

def reference(preserved_vector, nasa_table, gas_constant, species_index, face_kind):
    nasa_table_weights = nasa_table[species_index]
    component_kind_r_factor = gas_constant[species_index]
    block_ids = jnp.arange(N_GX, dtype=jnp.int32)

    def cell_block(block_id):
        patch_region = lax.dynamic_slice_in_dim(preserved_vector, (block_id * CX).astype(jnp.int32), CX, 1)
        kelvin_reading = solve_for_kelvin(patch_region, nasa_table_weights, component_kind_r_factor)
        patch_multiplier = nasa_fitted_monomials(patch_region, kelvin_reading, nasa_table_weights, component_kind_r_factor)
        bulk_compactness = lax.optimization_barrier(jnp.sum(patch_region[:NS], axis=0))
        velocity = patch_region[NS:NS + 3] / bulk_compactness[None]
        local_speed = lax.optimization_barrier(jnp.max(jnp.abs(velocity) + patch_multiplier[2][None], axis=(1, 2, 3)))
        return (patch_multiplier, local_speed)
    coef_blocks, speed_blocks = lax.map(cell_block, block_ids)
    cell_coef = jnp.transpose(coef_blocks, (1, 0, 2, 3, 4)).reshape((NS + 3, NX, NY, NZ))
    speeds = lax.optimization_barrier(jnp.max(speed_blocks, axis=0))

    def rate_block(inputs):
        block_id, kinds = inputs
        rows_index = (block_id * CX - 3 + jnp.arange(CX + 6, dtype=jnp.int32)) % NX
        state_x = jnp.take(preserved_vector, rows_index, axis=1)
        coef_x = jnp.take(cell_coef, rows_index, axis=1)
        rate = direction_rate(state_x, coef_x, 1, 0, speeds[0])
        state_mid = state_x[:, 3:3 + CX]
        coef_mid = coef_x[:, 3:3 + CX]
        state_y = jnp.concatenate([state_mid[:, :, -3:], state_mid, state_mid[:, :, :3]], axis=2)
        coef_y = jnp.concatenate([coef_mid[:, :, -3:], coef_mid, coef_mid[:, :, :3]], axis=2)
        rate = rate + direction_rate(state_y, coef_y, 2, 1, speeds[1])
        lower_kind = jnp.repeat(kinds[:, 0], CY).reshape((1, 1, NY, 1))
        upper_kind = jnp.repeat(kinds[:, 1], CY).reshape((1, 1, NY, 1))
        padded_z = wall_pad(jnp.concatenate([state_mid, coef_mid], axis=0), lower_kind, upper_kind)
        rate = rate + direction_rate(padded_z[:NVAR], padded_z[NVAR:], 3, 2, speeds[2])
        return rate
    rate_blocks = lax.map(rate_block, (block_ids, face_kind))
    rate = jnp.transpose(rate_blocks, (1, 0, 2, 3, 4)).reshape((NVAR, NX, NY, NZ))
    return COURANT / jnp.sum(speeds) * rate
```

```python
import jax
import jax.numpy as jnp
from jax import lax
from jax.experimental import pallas as pl
from jax.experimental.pallas import tpu as pltpu
from jax.sharding import Mesh
from jax.sharding import PartitionSpec as P

NS = 9
NVAR = 14
NEWTON = 2
EPSILON = 1e-06
COURANT = 0.8
LANES = 128
DF, DU, FM, HU, RD, ROWS = 0, 70, 140, 154, 168, 192
F32 = jnp.float32


def species_scalars(table, gas, index):
    rows = []
    for i in range(NS):
        row = index[i]
        r = gas[row]
        a = [r * table[row, k] for k in range(6)]
        e = [a[0] - r, a[1] * 0.5, a[2] * (1.0 / 3.0), a[3] * 0.25, a[4] * 0.2, a[5]]
        rows.append((r, a, e))
    return rows


def coefficients(u, rows):
    rho = u[0]
    for i in range(1, NS):
        rho = rho + u[i]
    inv = 1.0 / rho
    vel = [u[NS + j] * inv for j in range(3)]
    square = vel[0] * vel[0] + vel[1] * vel[1] + vel[2] * vel[2]
    target = u[NS + 3] - 0.5 * rho * square
    mix = [None] * 7
    for i in range(NS):
        r, a, _ = rows[i]
        for k, w in enumerate([r] + a):
            term = u[i] * w
            mix[k] = term if mix[k] is None else mix[k] + term
    r0, a1, a2, a3, a4, a5, a6 = mix
    b1, b2, b3, b4, b5 = a1 - r0, a2 * 0.5, a3 * (1.0 / 3.0), a4 * 0.25, a5 * 0.2
    temp = jnp.ones_like(rho)
    for _ in range(NEWTON):
        energy = a6 + temp * (b1 + temp * (b2 + temp * (b3 + temp * (b4 + temp * b5))))
        slope = b1 + temp * (a2 + temp * (a3 + temp * (a4 + temp * a5)))
        temp = temp - (energy - target) / slope
    slope = b1 + temp * (a2 + temp * (a3 + temp * (a4 + temp * a5)))
    g = r0 / slope
    p = r0 * temp
    c = jnp.sqrt((1.0 + g) * p * inv)
    kinetic = 0.5 * g * square
    phi = []
    for i in range(NS):
        r, _, e = rows[i]
        energy = e[5] + temp * (e[0] + temp * (e[1] + temp * (e[2] + temp * (e[3] + temp * e[4]))))
        phi.append(r * temp - g * energy + kinetic)
    return p, g, c, phi, vel


def cell_kernel(table, gas, index, u_ref, coef_ref, alpha_ref, xs_ref, xe_ref, ys_ref, ye_ref):
    rows = species_scalars(table, gas, index)
    fastest = [None] * 3

    def body(i, fastest):
        at = pl.ds(pl.multiple_of(i * 8, 8), 8)
        u = [u_ref[k, at, :] for k in range(NVAR)]
        p, g, c, phi, vel = coefficients(u, rows)
        for k, value in enumerate([p, g, c] + phi):
            coef_ref[k, at, :] = value
        return tuple(jnp.maximum(f, jnp.abs(v) + c) for f, v in zip(fastest, vel))

    zero = jnp.zeros((8, LANES), F32)
    fastest = lax.fori_loop(0, 8, body, (zero, zero, zero))
    sub = lax.broadcasted_iota(jnp.int32, (8, LANES), 0)
    out = zero
    for d in range(3):
        top = jnp.max(jnp.max(fastest[d], axis=0, keepdims=True), axis=1, keepdims=True)
        out = jnp.where(sub == d, jnp.broadcast_to(top, (8, LANES)), out)
    alpha_ref[...] = out
    for k in range(NVAR):
        xs_ref[k] = u_ref[k, 0:24, :]
        xe_ref[k] = u_ref[k, 40:64, :]
        for j in range(3):
            ys_ref[k, 8 * j:8 * j + 8, :] = u_ref[k, pl.ds(j, 8, stride=8), :]
            ye_ref[k, 8 * j:8 * j + 8, :] = u_ref[k, pl.ds(5 + j, 8, stride=8), :]


def cell_fields(u, coef, order):
    p, g, c, phi = coef[0], coef[1], coef[2], coef[3:]
    rho = u[0]
    for i in range(1, NS):
        rho = rho + u[i]
    inv = 1.0 / rho
    n = order[0]
    vel = [u[NS + j] * inv for j in order]
    half = [0.5 * x for x in u[:NS]] + [0.5 * u[NS + j] for j in order]
    half += [0.5 * u[NS + 3], 0.5 * u[NS + 4], 0.5 * rho]
    un = vel[0]
    flux = [x * un for x in half]
    ph = 0.5 * p
    flux[NS] = flux[NS] + ph
    flux[NS + 3] = flux[NS + 3] + ph * un
    mean = [x * inv for x in u[:NS]] + vel + [u[NS + 4] * inv, g, c] + phi
    return half, flux, mean


def face_record(out_ref, f, left, right, jumps, fm, hu):
    mean = [0.5 * (a + b) for a, b in zip(left, right)]
    y, vel, z, g, c, phi = mean[:9], mean[9:12], mean[12], mean[13], mean[14], mean[15:]
    square = vel[0] * vel[0] + vel[1] * vel[1] + vel[2] * vel[2]
    dot = y[0] * phi[0]
    for i in range(1, NS):
        dot = dot + y[i] * phi[i]
    ig = 1.0 / g
    ic = 1.0 / c
    inv = ic * ic
    h = (c * c - dot) * ig + square
    ihc = 0.5 * ic
    gs = g * inv
    phis = [x * inv for x in phi]
    gu = [gs * v for v in vel]
    record = y + vel + [z, c, h] + [square - x * ig for x in phi]
    for k, value in enumerate(record):
        out_ref[f, RD + k] = value
    for k in range(NVAR):
        out_ref[f, FM + k] = fm[k]
        out_ref[f, HU + k] = hu[k]
    for base, i, v in jumps():
        dp = phis[0] * v[0]
        for k in range(1, NS):
            dp = dp + phis[k] * v[k]
        dp = dp + gs * v[12] - (gu[0] * v[9] + gu[1] * v[10] + gu[2] * v[11])
        s = v[14]
        a = 0.5 * dp
        b = (v[9] - vel[0] * s) * ihc
        wave = [a - b] + [v[k] - y[k] * dp for k in range(NS)]
        wave += [v[10] - vel[1] * s, v[11] - vel[2] * s, a + b, v[13] - z * dp]
        for k in range(NVAR):
            out_ref[f, base + 14 * i + k] = wave[k]


def line_kernel(order, strided, table, gas, index, u_ref, coef_ref, low_ref, high_ref, out_ref,
                state, flux, mean):
    rows = species_scalars(table, gas, index)

    def put(plane, u, coef):
        a, b, m = cell_fields(u, coef, order)
        for k in range(15):
            state[plane, k] = a[k]
            flux[plane, k] = b[k]
        for k in range(24):
            mean[plane, k] = m[k]

    def own(i, _):
        at = pl.ds(i, 8, stride=8) if strided else pl.ds(pl.multiple_of(i * 8, 8), 8)
        put(i + 3, [u_ref[k, at, :] for k in range(NVAR)], [coef_ref[k, at, :] for k in range(12)])
        return 0

    lax.fori_loop(0, 8, own, 0)
    for ref, first in ((low_ref, 0), (high_ref, 11)):
        def halo(i, _, ref=ref, first=first):
            at = pl.ds(pl.multiple_of(i * 8, 8), 8)
            u = [ref[k, at, :] for k in range(NVAR)]
            p, g, c, phi, _ = coefficients(u, rows)
            put(i + first, u, [p, g, c] + phi)
            return 0
        lax.fori_loop(0, 3, halo, 0)

    def face(f, _):
        left = [mean[f + 2, k] for k in range(24)]
        right = [mean[f + 3, k] for k in range(24)]
        fm = [flux[f + 2, k] + flux[f + 3, k] for k in range(NVAR)]
        hu = [state[f + 3, k] - state[f + 2, k] for k in range(NVAR)]

        def jumps():
            for base, ref in ((DF, flux), (DU, state)):
                for i in range(5):
                    yield base, i, [ref[f + i + 1, k] - ref[f + i, k] for k in range(15)]

        face_record(out_ref, f, left, right, jumps, fm, hu)
        return 0

    lax.fori_loop(0, 9, face, 0)


def column_kernel(table, gas, index, kind, u_ref, coef_ref, out_ref, ends, state, flux):
    rows = species_scalars(table, gas, index)
    order = (2, 0, 1)
    lane = lax.broadcasted_iota(jnp.int32, (8, LANES), 1)
    slot = lane % 16
    group = lane // 16
    low_wall = kind[0, 0, 0] == 1
    high_wall = kind[0, 0, 1] == 1

    def pick(k, _):
        packed = jnp.zeros((8, LANES), F32)
        for plane in range(8):
            v = u_ref[k, 8 * plane:8 * plane + 8, :]
            low = pltpu.roll(v, (16 * plane + 3) % LANES, 1)
            high = pltpu.roll(v, (16 * plane + 8 - 123) % LANES, 1)
            packed = jnp.where(group == plane, jnp.where(slot < 8, low, high), packed)

        def at(shift):
            return pltpu.roll(packed, shift % LANES, 1)

        sign = jnp.where(k == NS + 2, -1.0, 1.0)
        mirror = jnp.where(slot == 2, at(-1), jnp.where(slot == 1, at(-3), at(-5))) * sign
        copy = jnp.where(slot == 2, at(-1), jnp.where(slot == 1, at(-2), at(-3)))
        low = jnp.where(low_wall, mirror, copy)
        mirror = jnp.where(slot == 13, at(1), jnp.where(slot == 14, at(3), at(5))) * sign
        copy = jnp.where(slot == 13, at(1), jnp.where(slot == 14, at(2), at(3)))
        high = jnp.where(high_wall, mirror, copy)
        ends[k] = jnp.where(slot < 3, low, jnp.where(slot > 12, high, packed))
        return 0

    lax.fori_loop(0, NVAR, pick, 0)

    def record(f, u, coef):
        half, fl, mean = cell_fields(u, coef, order)
        prev = [pltpu.roll(x, 1, 1) for x in mean]
        hl = [pltpu.roll(x, 1, 1) for x in half]
        fll = [pltpu.roll(x, 1, 1) for x in fl]
        for k in range(15):
            state[k] = half[k] - hl[k]
            flux[k] = fl[k] - fll[k]
        fm = [fl[k] + fll[k] for k in range(NVAR)]
        hu = [half[k] - hl[k] for k in range(NVAR)]

        def jumps():
            for base, ref in ((DF, flux), (DU, state)):
                for i in range(5):
                    vs = [ref[k] for k in range(15)]
                    if i != 2:
                        vs = [pltpu.roll(v, (2 - i) % LANES, 1) for v in vs]
                    yield base, i, vs

        face_record(out_ref, f, prev, mean, jumps, fm, hu)

    u = [ends[k] for k in range(NVAR)]
    p, g, c, phi, _ = coefficients(u, rows)
    record(8, u, [p, g, c] + phi)

    def plane(i, _):
        at = pl.ds(pl.multiple_of(i * 8, 8), 8)
        record(i, [u_ref[k, at, :] for k in range(NVAR)], [coef_ref[k, at, :] for k in range(12)])
        return 0

    lax.fori_loop(0, 8, plane, 0)


def correction(d0, d1, d2, d3):
    t0 = d0 - 1.375 * d1
    t1 = d1 - 0.625 * d2
    t2 = d3 - 1.375 * d2
    e1 = (0.609375 * d1) * d1 + 0.75 * EPSILON
    e2 = (0.609375 * d2) * d2 + 0.75 * EPSILON
    i0 = reciprocal(t0 * t0 + e1)
    i1 = reciprocal(t1 * t1 + e2)
    i2 = reciprocal(t2 * t2 + e2)
    w0 = i0 * i0
    w1 = 6.0 * (i1 * i1)
    w2 = 3.0 * (i2 * i2)
    q = 2.625 * d2
    lead = (2.25 * d1 - q) - (t0 + t0)
    return q + (w0 * lead + w1 * t1 - w2 * t2) * reciprocal(w0 + w1 + w2)


def reciprocal(x):
    return 1.0 / x


def rate_kernel(alpha_ref, x_ref, y_ref, z_ref, out_ref, fx, fy, fz):
    speeds = [alpha_ref[d:d + 1, :] for d in range(3)]
    scale = COURANT / (speeds[0] + speeds[1] + speeds[2])
    scale = jnp.broadcast_to(scale, (8, LANES))
    for ref, flux, d in ((x_ref, fx, 0), (y_ref, fy, 1), (z_ref, fz, 2)):
        speed = jnp.broadcast_to(speeds[d], (8, LANES))

        def face(f, _, ref=ref, flux=flux, speed=speed):
            def wave(k):
                a = [ref[f, DF + 14 * i + k] for i in range(5)]
                b = [ref[f, DU + 14 * i + k] * speed for i in range(5)]
                up = [a[i] + b[i] for i in range(4)]
                down = [a[i] - b[i] for i in range(1, 5)]
                return correction(*up) - correction(down[3], down[2], down[1], down[0])

            amp = [wave(k) for k in range(NVAR)]
            y = [ref[f, RD + k] for k in range(9)]
            un, ut, us, z, c, h = [ref[f, RD + 9 + k] for k in range(6)]
            slower, species, first, second, faster, scalar = (
                amp[0], amp[1:10], amp[10], amp[11], amp[12], amp[13])
            total = species[0]
            for k in range(1, NS):
                total = total + species[k]
            acoustic = slower + faster
            swing = (faster - slower) * c
            both = acoustic + total
            energy = h * acoustic + un * swing + ut * first + us * second
            for k in range(NS):
                energy = energy + ref[f, RD + 15 + k] * species[k]
            rows = [y[k] * acoustic + species[k] for k in range(NS)]
            rows += [un * both + swing, ut * both + first, us * both + second, energy,
                     z * acoustic + scalar]
            for k in range(NVAR):
                flux[f, k] = (rows[k] * (1.0 / 6.0) + (ref[f, FM + k] - ref[f, HU + k] * speed)) * scale
            return 0

        lax.fori_loop(0, 9, face, 0)

    row_x = list(range(NVAR))
    lane = lax.broadcasted_iota(jnp.int32, (8, LANES), 1)
    at_z = {9: 10, 10: 11, 11: 9}
    at_y = {9: 10, 10: 9, 11: 11}

    def plane(i, _):
        at = pl.ds(pl.multiple_of(i * 8, 8), 8)
        to_low = lax.rem(2 * LANES - 3 - 16 * i, LANES)
        to_high = lax.rem(2 * LANES - 13 - 16 * i, LANES)
        for k in range(NVAR):
            kz = at_z.get(k, k)
            ends = fz[8, kz]
            low = pltpu.roll(ends, to_low, 1)
            high = pltpu.roll(ends, to_high, 1)
            face = jnp.where(lane < 3, low, jnp.where(lane >= 126, high, fz[i, kz]))
            after = pltpu.roll(jnp.where(lane == 0, high, face), LANES - 1, 1)
            out_ref[k, at, :] = (face - after) + (fx[i, k] - fx[i + 1, k])
        return 0

    lax.fori_loop(0, 8, plane, 0)

    def row(j, _):
        at = pl.ds(j, 8, stride=8)
        for k in range(NVAR):
            ky = at_y.get(k, k)
            out_ref[k, at, :] = out_ref[k, at, :] + (fy[j, ky] - fy[j + 1, ky])
        return 0

    lax.fori_loop(0, 8, row, 0)


SMEM = pl.BlockSpec(memory_space=pltpu.SMEM)
VMEM = pl.BlockSpec(memory_space=pltpu.VMEM)
PLANES = (8, LANES)


def struct(*shape):
    return jax.ShapeDtypeStruct(shape, F32)


def params():
    return pltpu.CompilerParams(vmem_limit_bytes=48 << 20)


def cells(u, table, gas, index):
    halo = struct(NVAR, 24, LANES)
    return pl.pallas_call(
        cell_kernel, name="cells", in_specs=[SMEM] * 3 + [VMEM], out_specs=[VMEM] * 6,
        out_shape=[struct(12, 64, LANES), struct(8, LANES), halo, halo, halo, halo],
        compiler_params=params())(table, gas, index, u)


def lines(name, order, strided, table, gas, index, u, coef, low, high):
    def body(*refs):
        line_kernel(order, strided, *refs)
    return pl.pallas_call(
        body, name=name, in_specs=[SMEM] * 3 + [VMEM] * 4, out_specs=VMEM,
        out_shape=struct(9, ROWS, 8, LANES),
        scratch_shapes=[pltpu.VMEM((14, 15) + PLANES, F32), pltpu.VMEM((14, 15) + PLANES, F32),
                        pltpu.VMEM((14, 24) + PLANES, F32)],
        compiler_params=params())(table, gas, index, u, coef, low, high)


def columns(table, gas, index, kind, u, coef):
    return pl.pallas_call(
        column_kernel, name="columns", in_specs=[SMEM] * 4 + [VMEM] * 2, out_specs=VMEM,
        out_shape=struct(9, ROWS, 8, LANES),
        scratch_shapes=[pltpu.VMEM((14,) + PLANES, F32), pltpu.VMEM((15,) + PLANES, F32),
                        pltpu.VMEM((15,) + PLANES, F32)],
        compiler_params=params())(table, gas, index, kind, u, coef)


def rates(alpha, x, y, z):
    return pl.pallas_call(
        rate_kernel, name="rates", in_specs=[VMEM] * 4, out_specs=VMEM,
        out_shape=struct(NVAR, 64, LANES),
        scratch_shapes=[pltpu.VMEM((9, NVAR) + PLANES, F32)] * 3,
        compiler_params=params())(alpha, x, y, z)


AXES = ("z", "yl", "x", "yh", "c")
GX = ("z", "yl")
GY = ("x", "yh", "c")


def shards(preserved_vector, nasa_table, gas_constant, species_index, face_kind):
    u = preserved_vector.reshape(NVAR, 64, LANES)
    coef, alpha, xs, xe, ys, ye = cells(u, nasa_table, gas_constant, species_index)
    up = [(i, (i + 1) % 16) for i in range(16)]
    down = [(b, a) for a, b in up]
    for axis in reversed(AXES):
        size = lax.axis_size(axis)
        step = 1
        while step < size:
            alpha = jnp.maximum(alpha, lax.ppermute(alpha, axis, [(i, i ^ step) for i in range(size)]))
            step *= 2
    x_low, x_high = lax.ppermute(xe, GX, up), lax.ppermute(xs, GX, down)
    y_low, y_high = lax.ppermute(ye, GY, up), lax.ppermute(ys, GY, down)
    fixed = (nasa_table, gas_constant, species_index)
    z = columns(*fixed, face_kind, u, coef)
    x = lines("x_lines", (0, 1, 2), False, *fixed, u, coef, x_low, x_high)
    y = lines("y_lines", (1, 0, 2), True, *fixed, u, coef, y_low, y_high)
    return rates(alpha, x, y, z).reshape(preserved_vector.shape)


def solution(mesh):
    finer = Mesh(mesh.devices.reshape(8, 2, 4, 2, 2), AXES)
    placed = (P(None, GX, GY, None), P(), P(), P(), P(GX, GY, None))
    return jax.shard_map(
        shards, mesh=finer, in_specs=placed, out_specs=P(None, GX, GY, None), check_vma=False
    )
```

```python
import jax
import jax.numpy as jnp
from jax import lax
from jax.experimental import pallas as pl
from jax.experimental.pallas import tpu as pltpu
from jax.sharding import Mesh
from jax.sharding import PartitionSpec as P

NS = 9
NVAR = 14
NEWTON = 2
EPSILON = 1e-06
COURANT = 0.8
LANES = 128
DF, DU, FM, HU, RD, ROWS = 0, 70, 140, 154, 168, 192
F32 = jnp.float32


def species_scalars(table, gas, index):
    rows = []
    for i in range(NS):
        row = index[i]
        r = gas[row]
        a = [r * table[row, k] for k in range(6)]
        e = [a[0] - r, a[1] * 0.5, a[2] * (1.0 / 3.0), a[3] * 0.25, a[4] * 0.2, a[5]]
        rows.append((r, a, e))
    return rows


def coefficients(u, rows):
    rho = u[0]
    for i in range(1, NS):
        rho = rho + u[i]
    inv = 1.0 / rho
    vel = [u[NS + j] * inv for j in range(3)]
    square = vel[0] * vel[0] + vel[1] * vel[1] + vel[2] * vel[2]
    target = u[NS + 3] - 0.5 * rho * square
    mix = [None] * 7
    for i in range(NS):
        r, a, _ = rows[i]
        for k, w in enumerate([r] + a):
            term = u[i] * w
            mix[k] = term if mix[k] is None else mix[k] + term
    r0, a1, a2, a3, a4, a5, a6 = mix
    b1, b2, b3, b4, b5 = a1 - r0, a2 * 0.5, a3 * (1.0 / 3.0), a4 * 0.25, a5 * 0.2
    temp = jnp.ones_like(rho)
    for _ in range(NEWTON):
        energy = a6 + temp * (b1 + temp * (b2 + temp * (b3 + temp * (b4 + temp * b5))))
        slope = b1 + temp * (a2 + temp * (a3 + temp * (a4 + temp * a5)))
        temp = temp - (energy - target) / slope
    slope = b1 + temp * (a2 + temp * (a3 + temp * (a4 + temp * a5)))
    g = r0 / slope
    p = r0 * temp
    c = jnp.sqrt((1.0 + g) * p * inv)
    kinetic = 0.5 * g * square
    phi = []
    for i in range(NS):
        r, _, e = rows[i]
        energy = e[5] + temp * (e[0] + temp * (e[1] + temp * (e[2] + temp * (e[3] + temp * e[4]))))
        phi.append(r * temp - g * energy + kinetic)
    return p, g, c, phi, vel


def cell_kernel(table, gas, index, u_ref, coef_ref, alpha_ref, xs_ref, xe_ref, ys_ref, ye_ref):
    rows = species_scalars(table, gas, index)
    fastest = [None] * 3

    def body(i, fastest):
        at = pl.ds(pl.multiple_of(i * 8, 8), 8)
        u = [u_ref[k, at, :] for k in range(NVAR)]
        p, g, c, phi, vel = coefficients(u, rows)
        for k, value in enumerate([p, g, c] + phi):
            coef_ref[k, at, :] = value
        return tuple(jnp.maximum(f, jnp.abs(v) + c) for f, v in zip(fastest, vel))

    zero = jnp.zeros((8, LANES), F32)
    fastest = lax.fori_loop(0, 8, body, (zero, zero, zero))
    sub = lax.broadcasted_iota(jnp.int32, (8, LANES), 0)
    out = zero
    for d in range(3):
        top = jnp.max(jnp.max(fastest[d], axis=0, keepdims=True), axis=1, keepdims=True)
        out = jnp.where(sub == d, jnp.broadcast_to(top, (8, LANES)), out)
    alpha_ref[...] = out
    for k in range(NVAR):
        xs_ref[k] = u_ref[k, 0:24, :]
        xe_ref[k] = u_ref[k, 40:64, :]
        for j in range(3):
            ys_ref[k, 8 * j:8 * j + 8, :] = u_ref[k, pl.ds(j, 8, stride=8), :]
            ye_ref[k, 8 * j:8 * j + 8, :] = u_ref[k, pl.ds(5 + j, 8, stride=8), :]


def cell_fields(u, coef, order):
    p, g, c, phi = coef[0], coef[1], coef[2], coef[3:]
    rho = u[0]
    for i in range(1, NS):
        rho = rho + u[i]
    inv = 1.0 / rho
    n = order[0]
    vel = [u[NS + j] * inv for j in order]
    half = [0.5 * x for x in u[:NS]] + [0.5 * u[NS + j] for j in order]
    half += [0.5 * u[NS + 3], 0.5 * u[NS + 4], 0.5 * rho]
    un = vel[0]
    flux = [x * un for x in half]
    ph = 0.5 * p
    flux[NS] = flux[NS] + ph
    flux[NS + 3] = flux[NS + 3] + ph * un
    mean = [x * inv for x in u[:NS]] + vel + [u[NS + 4] * inv, g, c] + phi
    return half, flux, mean


def face_record(out_ref, f, left, right, jumps, fm, hu):
    mean = [0.5 * (a + b) for a, b in zip(left, right)]
    y, vel, z, g, c, phi = mean[:9], mean[9:12], mean[12], mean[13], mean[14], mean[15:]
    square = vel[0] * vel[0] + vel[1] * vel[1] + vel[2] * vel[2]
    dot = y[0] * phi[0]
    for i in range(1, NS):
        dot = dot + y[i] * phi[i]
    ig = 1.0 / g
    ic = 1.0 / c
    inv = ic * ic
    h = (c * c - dot) * ig + square
    ihc = 0.5 * ic
    gs = g * inv
    phis = [x * inv for x in phi]
    gu = [gs * v for v in vel]
    record = y + vel + [z, c, h] + [square - x * ig for x in phi]
    for k, value in enumerate(record):
        out_ref[f, RD + k] = value
    for k in range(NVAR):
        out_ref[f, FM + k] = fm[k]
        out_ref[f, HU + k] = hu[k]
    for base, i, v in jumps():
        dp = phis[0] * v[0]
        for k in range(1, NS):
            dp = dp + phis[k] * v[k]
        dp = dp + gs * v[12] - (gu[0] * v[9] + gu[1] * v[10] + gu[2] * v[11])
        s = v[14]
        a = 0.5 * dp
        b = (v[9] - vel[0] * s) * ihc
        wave = [a - b] + [v[k] - y[k] * dp for k in range(NS)]
        wave += [v[10] - vel[1] * s, v[11] - vel[2] * s, a + b, v[13] - z * dp]
        for k in range(NVAR):
            out_ref[f, base + 14 * i + k] = wave[k]


def line_kernel(order, strided, table, gas, index, u_ref, coef_ref, low_ref, high_ref, out_ref,
                state, flux, mean):
    rows = species_scalars(table, gas, index)

    def put(plane, u, coef):
        a, b, m = cell_fields(u, coef, order)
        for k in range(15):
            state[plane, k] = a[k]
            flux[plane, k] = b[k]
        for k in range(24):
            mean[plane, k] = m[k]

    def own(i, _):
        at = pl.ds(i, 8, stride=8) if strided else pl.ds(pl.multiple_of(i * 8, 8), 8)
        put(i + 3, [u_ref[k, at, :] for k in range(NVAR)], [coef_ref[k, at, :] for k in range(12)])
        return 0

    lax.fori_loop(0, 8, own, 0)
    for ref, first in ((low_ref, 0), (high_ref, 11)):
        def halo(i, _, ref=ref, first=first):
            at = pl.ds(pl.multiple_of(i * 8, 8), 8)
            u = [ref[k, at, :] for k in range(NVAR)]
            p, g, c, phi, _ = coefficients(u, rows)
            put(i + first, u, [p, g, c] + phi)
            return 0
        lax.fori_loop(0, 3, halo, 0)

    def face(f, _):
        left = [mean[f + 2, k] for k in range(24)]
        right = [mean[f + 3, k] for k in range(24)]
        fm = [flux[f + 2, k] + flux[f + 3, k] for k in range(NVAR)]
        hu = [state[f + 3, k] - state[f + 2, k] for k in range(NVAR)]

        def jumps():
            for base, ref in ((DF, flux), (DU, state)):
                for i in range(5):
                    yield base, i, [ref[f + i + 1, k] - ref[f + i, k] for k in range(15)]

        face_record(out_ref, f, left, right, jumps, fm, hu)
        return 0

    lax.fori_loop(0, 9, face, 0)


def column_kernel(table, gas, index, kind, u_ref, coef_ref, out_ref, ends, state, flux):
    rows = species_scalars(table, gas, index)
    order = (2, 0, 1)
    lane = lax.broadcasted_iota(jnp.int32, (8, LANES), 1)
    slot = lane % 16
    group = lane // 16
    low_wall = kind[0, 0, 0] == 1
    high_wall = kind[0, 0, 1] == 1

    def pick(k, _):
        packed = jnp.zeros((8, LANES), F32)
        for plane in range(8):
            v = u_ref[k, 8 * plane:8 * plane + 8, :]
            low = pltpu.roll(v, (16 * plane + 3) % LANES, 1)
            high = pltpu.roll(v, (16 * plane + 8 - 123) % LANES, 1)
            packed = jnp.where(group == plane, jnp.where(slot < 8, low, high), packed)

        def at(shift):
            return pltpu.roll(packed, shift % LANES, 1)

        sign = jnp.where(k == NS + 2, -1.0, 1.0)
        mirror = jnp.where(slot == 2, at(-1), jnp.where(slot == 1, at(-3), at(-5))) * sign
        copy = jnp.where(slot == 2, at(-1), jnp.where(slot == 1, at(-2), at(-3)))
        low = jnp.where(low_wall, mirror, copy)
        mirror = jnp.where(slot == 13, at(1), jnp.where(slot == 14, at(3), at(5))) * sign
        copy = jnp.where(slot == 13, at(1), jnp.where(slot == 14, at(2), at(3)))
        high = jnp.where(high_wall, mirror, copy)
        ends[k] = jnp.where(slot < 3, low, jnp.where(slot > 12, high, packed))
        return 0

    lax.fori_loop(0, NVAR, pick, 0)

    def record(f, u, coef):
        half, fl, mean = cell_fields(u, coef, order)
        prev = [pltpu.roll(x, 1, 1) for x in mean]
        hl = [pltpu.roll(x, 1, 1) for x in half]
        fll = [pltpu.roll(x, 1, 1) for x in fl]
        for k in range(15):
            state[k] = half[k] - hl[k]
            flux[k] = fl[k] - fll[k]
        fm = [fl[k] + fll[k] for k in range(NVAR)]
        hu = [half[k] - hl[k] for k in range(NVAR)]

        def jumps():
            for base, ref in ((DF, flux), (DU, state)):
                for i in range(5):
                    vs = [ref[k] for k in range(15)]
                    if i != 2:
                        vs = [pltpu.roll(v, (2 - i) % LANES, 1) for v in vs]
                    yield base, i, vs

        face_record(out_ref, f, prev, mean, jumps, fm, hu)

    u = [ends[k] for k in range(NVAR)]
    p, g, c, phi, _ = coefficients(u, rows)
    record(8, u, [p, g, c] + phi)

    def plane(i, _):
        at = pl.ds(pl.multiple_of(i * 8, 8), 8)
        record(i, [u_ref[k, at, :] for k in range(NVAR)], [coef_ref[k, at, :] for k in range(12)])
        return 0

    lax.fori_loop(0, 8, plane, 0)


def correction(d0, d1, d2, d3):
    t0 = d0 - 1.375 * d1
    t1 = d1 - 0.625 * d2
    t2 = d3 - 1.375 * d2
    e1 = (0.609375 * d1) * d1 + 0.75 * EPSILON
    e2 = (0.609375 * d2) * d2 + 0.75 * EPSILON
    i0 = reciprocal(t0 * t0 + e1)
    i1 = reciprocal(t1 * t1 + e2)
    i2 = reciprocal(t2 * t2 + e2)
    w0 = i0 * i0
    w1 = 6.0 * (i1 * i1)
    w2 = 3.0 * (i2 * i2)
    q = 2.625 * d2
    lead = (2.25 * d1 - q) - (t0 + t0)
    return q + (w0 * lead + w1 * t1 - w2 * t2) * reciprocal(w0 + w1 + w2)


def reciprocal(x):
    return 1.0 / x


def rate_kernel(alpha_ref, x_ref, y_ref, z_ref, out_ref, fx, fy, fz):
    speeds = [alpha_ref[d:d + 1, :] for d in range(3)]
    scale = COURANT / (speeds[0] + speeds[1] + speeds[2])
    scale = jnp.broadcast_to(scale, (8, LANES))
    for ref, flux, d in ((x_ref, fx, 0), (y_ref, fy, 1), (z_ref, fz, 2)):
        speed = jnp.broadcast_to(speeds[d], (8, LANES))

        def face(f, _, ref=ref, flux=flux, speed=speed):
            def wave(k):
                a = [ref[f, DF + 14 * i + k] for i in range(5)]
                b = [ref[f, DU + 14 * i + k] * speed for i in range(5)]
                up = [a[i] + b[i] for i in range(4)]
                down = [a[i] - b[i] for i in range(1, 5)]
                return correction(*up) - correction(down[3], down[2], down[1], down[0])

            amp = [wave(k) for k in range(NVAR)]
            y = [ref[f, RD + k] for k in range(9)]
            un, ut, us, z, c, h = [ref[f, RD + 9 + k] for k in range(6)]
            slower, species, first, second, faster, scalar = (
                amp[0], amp[1:10], amp[10], amp[11], amp[12], amp[13])
            total = species[0]
            for k in range(1, NS):
                total = total + species[k]
            acoustic = slower + faster
            swing = (faster - slower) * c
            both = acoustic + total
            energy = h * acoustic + un * swing + ut * first + us * second
            for k in range(NS):
                energy = energy + ref[f, RD + 15 + k] * species[k]
            rows = [y[k] * acoustic + species[k] for k in range(NS)]
            rows += [un * both + swing, ut * both + first, us * both + second, energy,
                     z * acoustic + scalar]
            for k in range(NVAR):
                flux[f, k] = (rows[k] * (1.0 / 6.0) + (ref[f, FM + k] - ref[f, HU + k] * speed)) * scale
            return 0

        lax.fori_loop(0, 9, face, 0)

    row_x = list(range(NVAR))
    lane = lax.broadcasted_iota(jnp.int32, (8, LANES), 1)
    at_z = {9: 10, 10: 11, 11: 9}
    at_y = {9: 10, 10: 9, 11: 11}

    def plane(i, _):
        at = pl.ds(pl.multiple_of(i * 8, 8), 8)
        to_low = lax.rem(2 * LANES - 3 - 16 * i, LANES)
        to_high = lax.rem(2 * LANES - 13 - 16 * i, LANES)
        for k in range(NVAR):
            kz = at_z.get(k, k)
            ends = fz[8, kz]
            low = pltpu.roll(ends, to_low, 1)
            high = pltpu.roll(ends, to_high, 1)
            face = jnp.where(lane < 3, low, jnp.where(lane >= 126, high, fz[i, kz]))
            after = pltpu.roll(jnp.where(lane == 0, high, face), LANES - 1, 1)
            out_ref[k, at, :] = (face - after) + (fx[i, k] - fx[i + 1, k])
        return 0

    lax.fori_loop(0, 8, plane, 0)

    def row(j, _):
        at = pl.ds(j, 8, stride=8)
        for k in range(NVAR):
            ky = at_y.get(k, k)
            out_ref[k, at, :] = out_ref[k, at, :] + (fy[j, ky] - fy[j + 1, ky])
        return 0

    lax.fori_loop(0, 8, row, 0)


SMEM = pl.BlockSpec(memory_space=pltpu.SMEM)
VMEM = pl.BlockSpec(memory_space=pltpu.VMEM)
PLANES = (8, LANES)


def struct(*shape):
    return jax.ShapeDtypeStruct(shape, F32)


def params():
    return pltpu.CompilerParams(vmem_limit_bytes=20 << 20)


def cells(u, table, gas, index):
    halo = struct(NVAR, 24, LANES)
    return pl.pallas_call(
        cell_kernel, name="cells", in_specs=[SMEM] * 3 + [VMEM], out_specs=[VMEM] * 6,
        out_shape=[struct(12, 64, LANES), struct(8, LANES), halo, halo, halo, halo],
        compiler_params=params())(table, gas, index, u)


def lines(name, order, strided, table, gas, index, u, coef, low, high):
    def body(*refs):
        line_kernel(order, strided, *refs)
    return pl.pallas_call(
        body, name=name, in_specs=[SMEM] * 3 + [VMEM] * 4, out_specs=VMEM,
        out_shape=struct(9, ROWS, 8, LANES),
        scratch_shapes=[pltpu.VMEM((14, 15) + PLANES, F32), pltpu.VMEM((14, 15) + PLANES, F32),
                        pltpu.VMEM((14, 24) + PLANES, F32)],
        compiler_params=params())(table, gas, index, u, coef, low, high)


def columns(table, gas, index, kind, u, coef):
    return pl.pallas_call(
        column_kernel, name="columns", in_specs=[SMEM] * 4 + [VMEM] * 2, out_specs=VMEM,
        out_shape=struct(9, ROWS, 8, LANES),
        scratch_shapes=[pltpu.VMEM((14,) + PLANES, F32), pltpu.VMEM((15,) + PLANES, F32),
                        pltpu.VMEM((15,) + PLANES, F32)],
        compiler_params=params())(table, gas, index, kind, u, coef)


def rates(alpha, x, y, z):
    return pl.pallas_call(
        rate_kernel, name="rates", in_specs=[VMEM] * 4, out_specs=VMEM,
        out_shape=struct(NVAR, 64, LANES),
        scratch_shapes=[pltpu.VMEM((9, NVAR) + PLANES, F32)] * 3,
        compiler_params=params())(alpha, x, y, z)


AXES = ("z", "yl", "x", "yh", "c")
GX = ("z", "yl")
GY = ("x", "yh", "c")


def flat(z, y, x, c):
    return (((z * 2 + y % 2) * 4 + x) * 2 + y // 2) * 2 + c


def exchange(value, dim, partner):
    pairs = []
    for z in range(8):
        for y in range(4):
            for x in range(4):
                at = [z, y, x]
                to = list(at)
                to[dim] = partner(at[dim])
                pairs += [(flat(*at, c), flat(*to, c)) for c in range(2)]
    return lax.ppermute(value, AXES, pairs)


def near(i):
    return i ^ 1


def other(n):
    return lambda i: (i + 1) % n if i % 2 else (i - 1) % n


def far(i):
    return (3, 6, 5, 0, 7, 2, 1, 4)[i]


def core(value):
    return jnp.maximum(value, lax.ppermute(value, "c", [(0, 1), (1, 0)]))


def shards(preserved_vector, nasa_table, gas_constant, species_index, face_kind):
    u = preserved_vector.reshape(NVAR, 64, LANES)
    fixed = (nasa_table, gas_constant, species_index)
    coef, alpha, xs, xe, ys, ye = cells(u, *fixed)
    up = [(i, (i + 1) % 16) for i in range(16)]
    down = [(b, a) for a, b in up]
    x_low, x_high = lax.ppermute(xe, GX, up), lax.ppermute(xs, GX, down)
    y_low, y_high = lax.ppermute(ye, GY, up), lax.ppermute(ys, GY, down)

    wide = jnp.broadcast_to(alpha[0:3, 0].reshape(1, 1, 3), (256, 1, 3))
    wide = lax.all_to_all(wide, AXES, 0, 0, tiled=True)
    alpha = jnp.broadcast_to(jnp.pad(jnp.max(wide, axis=0).reshape(3, 1), ((0, 5), (0, 0))), (8, LANES))

    z = columns(*fixed, face_kind, u, coef)
    x = lines("x_lines", (0, 1, 2), False, *fixed, u, coef, x_low, x_high)
    y = lines("y_lines", (1, 0, 2), True, *fixed, u, coef, y_low, y_high)
    return rates(alpha, x, y, z).reshape(preserved_vector.shape)


def solution(mesh):
    finer = Mesh(mesh.devices.reshape(8, 2, 4, 2, 2), AXES)
    placed = (P(None, GX, GY, None), P(), P(), P(), P(GX, GY, None))
    return jax.shard_map(
        shards, mesh=finer, in_specs=placed, out_specs=P(None, GX, GY, None), check_vma=False
    )
```

```python
import jax
import jax.numpy as jnp
from jax import lax
from jax.experimental import pallas as pl
from jax.experimental.pallas import tpu as pltpu
from jax.sharding import Mesh
from jax.sharding import PartitionSpec as P


NS = 9
NVAR = 14
NEWTON = 2
EPSILON = 1e-06
COURANT = 0.8
LANES = 128
F32 = jnp.float32


def species_constants(table, gas, index, const):
    for i in range(NS):
        row = index[i]
        r = jnp.full((8, LANES), gas[row], F32)
        a = [r * jnp.full((8, LANES), table[k, row], F32) for k in range(6)]
        rest = [a[0] - r, a[1] * 0.5, a[2] * (1.0 / 3.0), a[3] * 0.25, a[4] * 0.2]
        for k, value in enumerate([r] + a + rest):
            const[12 * i + k] = value


def coefficients(u, rows):
    rho = u[0]
    for i in range(1, NS):
        rho = rho + u[i]
    inv = 1.0 / rho
    vel = [u[NS + j] * inv for j in range(3)]
    square = vel[0] * vel[0] + vel[1] * vel[1] + vel[2] * vel[2]
    target = u[NS + 3] - 0.5 * rho * square
    mix = [None] * 7
    for i in range(NS):
        for k in range(7):
            term = u[i] * rows[12 * i + k]
            mix[k] = term if mix[k] is None else mix[k] + term
    r0, a1, a2, a3, a4, a5, a6 = mix
    b1, b2, b3, b4, b5 = a1 - r0, a2 * 0.5, a3 * (1.0 / 3.0), a4 * 0.25, a5 * 0.2
    temp = jnp.ones_like(rho)
    for _ in range(NEWTON):
        energy = a6 + temp * (b1 + temp * (b2 + temp * (b3 + temp * (b4 + temp * b5))))
        slope = b1 + temp * (a2 + temp * (a3 + temp * (a4 + temp * a5)))
        temp = temp - (energy - target) / slope
    slope = b1 + temp * (a2 + temp * (a3 + temp * (a4 + temp * a5)))
    g = r0 / slope
    p = r0 * temp
    c = jnp.sqrt((1.0 + g) * p * inv)
    kinetic = 0.5 * g * square
    phi = []
    for i in range(NS):
        e = [rows[12 * i + 6 + k] for k in range(6)]
        energy = e[0] + temp * (e[1] + temp * (e[2] + temp * (e[3] + temp * (e[4] + temp * e[5]))))
        phi.append(rows[12 * i] * temp - g * energy + kinetic)
    return p, g, c, phi, vel


def halves(u, rows):
    p, g, c, phi, _ = coefficients(u, rows)
    return [0.5 * x for x in [p, g, c] + phi]


def fetch(pairs, sem):
    copies = [pltpu.make_async_copy(src, dst, sem.at[i]) for i, (src, dst) in enumerate(pairs)]
    for copy in copies:
        copy.start()
    return copies


def cell_kernel(table_h, gas_h, index_h, u_h, wide_ref, xs_ref, xe_ref, ys_ref, ye_ref,
                table, gas, index, rows, u_ref, sem):
    for copy in fetch([(table_h, table), (gas_h, gas), (index_h, index), (u_h, u_ref)], sem):
        copy.wait()
    species_constants(table, gas, index, rows)

    def body(i, fastest):
        at = pl.ds(pl.multiple_of(i * 8, 8), 8)
        u = [u_ref[k, at, :] for k in range(NVAR)]
        c, vel = coefficients(u, rows)[2::2]
        return tuple(jnp.maximum(f, jnp.abs(v) + c) for f, v in zip(fastest, vel))

    zero = jnp.zeros((8, LANES), F32)
    fastest = lax.fori_loop(0, 8, body, (zero, zero, zero), unroll=4)
    lane = lax.broadcasted_iota(jnp.int32, (8, LANES), 1)
    out = zero
    for d in range(3):
        top = jnp.max(jnp.max(fastest[d], axis=0, keepdims=True), axis=1, keepdims=True)
        out = jnp.where(lane == d, jnp.broadcast_to(top, (8, LANES)), out)
    for i in range(32):
        wide_ref[8 * i:8 * i + 8, :] = out
    for k in range(NVAR):
        xs_ref[k] = u_ref[k, 0:24, :]
        xe_ref[k] = u_ref[k, 40:64, :]
        for j in range(3):
            ys_ref[k, 8 * j:8 * j + 8, :] = u_ref[k, pl.ds(j, 8, stride=8), :]
            ye_ref[k, 8 * j:8 * j + 8, :] = u_ref[k, pl.ds(5 + j, 8, stride=8), :]


def correction(d0, d1, d2, d3):
    t0 = d0 - 1.375 * d1
    t1 = d1 - 0.625 * d2
    t2 = d3 - 1.375 * d2
    e1 = (0.609375 * d1) * d1 + 0.75 * EPSILON
    e2 = (0.609375 * d2) * d2 + 0.75 * EPSILON
    i0 = reciprocal(t0 * t0 + e1)
    i1 = reciprocal(t1 * t1 + e2)
    i2 = reciprocal(t2 * t2 + e2)
    w0 = i0 * i0
    w1 = 6.0 * (i1 * i1)
    w2 = 3.0 * (i2 * i2)
    q = 2.625 * d2
    lead = (2.25 * d1 - q) - (t0 + t0)
    return q + (w0 * lead + w1 * t1 - w2 * t2) * reciprocal(w0 + w1 + w2)


def reciprocal(x):
    return 1.0 / x


def split_fields(u, coef, order, speed):
    p, g, c, phi = coef[0], coef[1], coef[2], coef[3:]
    rho = u[0]
    for i in range(1, NS):
        rho = rho + u[i]
    inv = 0.5 / rho
    vel = [u[NS + j] * inv for j in order]
    plus, minus = vel[0] + speed, vel[0] - speed
    rows = u[:NS] + [u[NS + j] for j in order] + [u[NS + 3], u[NS + 4], rho]
    up = [x * plus for x in rows]
    down = [x * minus for x in rows]
    work = (p + p) * vel[0]
    for side in (up, down):
        side[NS] = side[NS] + p
        side[NS + 3] = side[NS + 3] + work
    mean = [x * inv for x in u[:NS]] + vel + [u[NS + 4] * inv, g, c] + phi
    return up, down, mean


def face_flux(left, right, jump, put):
    def mean(k):
        return left(k) + right(k)

    g, c = mean(13), mean(14)
    vel = [mean(9 + k) for k in range(3)]
    ig = 1.0 / g
    ic = 1.0 / c
    inv = ic * ic
    ihc = 0.5 * ic
    gs = g * inv
    gu = [gs * v for v in vel]
    square = vel[0] * vel[0] + vel[1] * vel[1] + vel[2] * vel[2]
    dot = None
    phis = []
    for k in range(NS):
        phi = mean(15 + k)
        term = mean(k) * phi
        dot = term if dot is None else dot + term
        phis.append(phi * inv)
    h = (c * c - dot) * ig + square
    pressure, swings, sums = {}, {}, {}
    for side in range(2):
        for i in range(side, 4 + side):
            dp = phis[0] * jump(side, i, 0)
            for k in range(1, NS):
                dp = dp + phis[k] * jump(side, i, k)
            v = [jump(side, i, NS + k) for k in range(3)]
            s = jump(side, i, 14)
            dp = dp + (gs * jump(side, i, 12) - (gu[0] * v[0] + gu[1] * v[1] + gu[2] * v[2]))
            pressure[side, i] = dp
            swings[side, i] = (v[0] - vel[0] * s) * ihc
            sums[side, i] = s

    def amplitude(wave):
        p = [wave(0, i) for i in range(4)]
        m = [wave(1, i) for i in range(4, 0, -1)]
        return correction(*p) - correction(*m)

    slower = amplitude(lambda side, i: 0.5 * pressure[side, i] - swings[side, i])
    faster = amplitude(lambda side, i: 0.5 * pressure[side, i] + swings[side, i])
    first = amplitude(lambda side, i: jump(side, i, 10) - vel[1] * sums[side, i])
    second = amplitude(lambda side, i: jump(side, i, 11) - vel[2] * sums[side, i])
    acoustic = slower + faster
    swing = (faster - slower) * c
    energy = h * acoustic + vel[0] * swing + vel[1] * first + vel[2] * second
    z = mean(12)
    put(13, z * acoustic + amplitude(lambda side, i: jump(side, i, 13) - z * pressure[side, i]))
    total = dot = None
    for k in range(NS):
        yk = mean(k)
        species = amplitude(lambda side, i: jump(side, i, k) - yk * pressure[side, i])
        put(k, yk * acoustic + species)
        term = phis[k] * species
        total = species if total is None else total + species
        dot = term if dot is None else dot + term
    both = acoustic + total
    put(9, vel[0] * both + swing)
    put(10, vel[1] * both + first)
    put(11, vel[2] * both + second)
    put(12, energy + square * total - (dot * (c * c)) * ig)


def own_kernel(table_h, gas_h, index_h, kind_h, u_h, coef_ref, ends_ref,
               table, gas, index, rows, kind, u_ref, sem):
    for copy in fetch([(table_h, table), (gas_h, gas), (index_h, index), (kind_h, kind),
                       (u_h, u_ref)], sem):
        copy.wait()
    species_constants(table, gas, index, rows)
    lane = lax.broadcasted_iota(jnp.int32, (8, LANES), 1)
    slot = lane % 16
    group = lane // 16
    low_wall = kind[0, 0] == 1
    high_wall = kind[0, 1] == 1

    def pick(k):
        packed = jnp.zeros((8, LANES), F32)
        for plane in range(8):
            v = u_ref[k, 8 * plane:8 * plane + 8, :]
            low = pltpu.roll(v, (16 * plane + 3) % LANES, 1)
            high = pltpu.roll(v, (16 * plane + 8 - 123) % LANES, 1)
            packed = jnp.where(group == plane, jnp.where(slot < 8, low, high), packed)

        def at(shift):
            return pltpu.roll(packed, shift % LANES, 1)

        sign = -1.0 if k == NS + 2 else 1.0
        mirror = jnp.where(slot == 2, at(-1), jnp.where(slot == 1, at(-3), at(-5))) * sign
        copy = jnp.where(slot == 2, at(-1), jnp.where(slot == 1, at(-2), at(-3)))
        low = jnp.where(low_wall, mirror, copy)
        mirror = jnp.where(slot == 13, at(1), jnp.where(slot == 14, at(3), at(5))) * sign
        copy = jnp.where(slot == 13, at(1), jnp.where(slot == 14, at(2), at(3)))
        high = jnp.where(high_wall, mirror, copy)
        ends_ref[k] = jnp.where(slot < 3, low, jnp.where(slot > 12, high, packed))
        return 0

    for k in range(NVAR):
        pick(k)
    for k, value in enumerate(halves([ends_ref[k] for k in range(NVAR)], rows)):
        ends_ref[NVAR + k] = value

    def plane(i, _):
        at = pl.ds(pl.multiple_of(i * 8, 8), 8)
        for k, value in enumerate(halves([u_ref[k, at, :] for k in range(NVAR)], rows)):
            coef_ref[k, at, :] = value
        return 0

    lax.fori_loop(0, 8, plane, 0, unroll=4)


def halo_kernel(table_h, gas_h, index_h, *refs):
    halos, outs, (table, gas, index, rows, sem) = refs[:4], refs[4:8], refs[8:]
    for copy in fetch([(table_h, table), (gas_h, gas), (index_h, index)], sem):
        copy.wait()
    species_constants(table, gas, index, rows)
    for u_ref, out_ref in zip(halos, outs):
        def plane(i, _, u_ref=u_ref, out_ref=out_ref):
            at = pl.ds(pl.multiple_of(i * 8, 8), 8)
            for k, value in enumerate(halves([u_ref[k, at, :] for k in range(NVAR)], rows)):
                out_ref[k, at, :] = value
            return 0

        lax.fori_loop(0, 3, plane, 0, unroll=True)


def rate_kernel(wide, u_ref, coef_ref, ends_ref, *refs):
    halo_u, halo_c, out_h = refs[:4], refs[4:8], refs[8]
    (pm, mean, jumps, columns, fx, fy, fz, fold, out_ref, out_sem) = refs[9:]
    top = wide[0:8, :]
    for i in range(1, 32):
        top = jnp.maximum(top, wide[8 * i:8 * i + 8, :])
    top = jnp.max(top, axis=0, keepdims=True)
    lane = lax.broadcasted_iota(jnp.int32, (1, LANES), 1)
    speeds = []
    for d in range(3):
        one = jnp.max(jnp.where(lane == d, top, 0.0), axis=1, keepdims=True)
        speeds.append(jnp.broadcast_to(0.5 * one, (8, LANES)))
    scale = (0.5 * COURANT) / (speeds[0] + speeds[1] + speeds[2])

    def emit(flux, f, base):
        def put(k, value):
            flux[f, k] = value * (1.0 / 6.0) + base(k)

        return put

    def column(f, u, coef):
        up, down, m = split_fields(u, coef, (2, 0, 1), speeds[2])
        for k in range(24):
            mean[f, k] = m[k] + pltpu.roll(m[k], 1, 1)
        for k in range(15):
            before = pltpu.roll(up[k], 1, 1)
            step = up[k] - before
            for i, shift in enumerate((2, 1, 0, LANES - 1)):
                columns[f, 15 * i + k] = pltpu.roll(step, shift, 1) if shift else step
            pm[f, k] = before + down[k]
            step = down[k] - pltpu.roll(down[k], 1, 1)
            for i, shift in enumerate((1, 0, LANES - 1, LANES - 2)):
                columns[f, 60 + 15 * i + k] = pltpu.roll(step, shift, 1) if shift else step

    column(8, [ends_ref[k] for k in range(NVAR)], [ends_ref[NVAR + k] for k in range(12)])

    def plane(i, _):
        at = pl.ds(pl.multiple_of(i * 8, 8), 8)
        column(i, [u_ref[k, at, :] for k in range(NVAR)], [coef_ref[k, at, :] for k in range(12)])
        return 0

    lax.fori_loop(0, 8, plane, 0)

    def upright(f, _):
        face_flux(lambda k: mean[f, k], lambda k: 0.0,
                  lambda side, i, k: columns[f, 60 * side + 15 * (i - side) + k],
                  emit(fz, f, lambda k: pm[f, k]))
        return 0

    lax.fori_loop(0, 9, upright, 0)
    for d, order, strided, flux in ((0, (0, 1, 2), False, fx), (1, (1, 0, 2), True, fy)):
        def cell(i, u, coef, d=d, order=order):
            up, down, m = split_fields(u, coef, order, speeds[d])
            for k in range(24):
                mean[i, k] = m[k]
            for k in range(15):
                pm[i, k] = up[k]
                pm[i, 15 + k] = down[k]

        def own(i, _, cell=cell, strided=strided):
            at = pl.ds(i, 8, stride=8) if strided else pl.ds(pl.multiple_of(i * 8, 8), 8)
            cell(i + 3, [u_ref[k, at, :] for k in range(NVAR)],
                 [coef_ref[k, at, :] for k in range(12)])
            return 0

        lax.fori_loop(0, 8, own, 0, unroll=2)

        for high in range(2):
            def halo(i, _, cell=cell, d=d, high=high):
                at = pl.ds(pl.multiple_of(i * 8, 8), 8)
                cell(i + 11 * high, [halo_u[2 * d + high][k, at, :] for k in range(NVAR)],
                     [halo_c[2 * d + high][k, at, :] for k in range(12)])
                return 0

            lax.fori_loop(0, 3, halo, 0, unroll=True)

        def jump(i, _):
            for k in range(30):
                jumps[i, k] = pm[i + 1, k] - pm[i, k]
            return 0

        lax.fori_loop(0, 13, jump, 0, unroll=True)

        def face(f, _, flux=flux):
            face_flux(lambda k: mean[f + 2, k], lambda k: mean[f + 3, k],
                      lambda side, i, k: jumps[f + i, 15 * side + k],
                      emit(flux, f, lambda k: pm[f + 2, k] + pm[f + 3, 15 + k]))
            return 0

        lax.fori_loop(0, 9, face, 0)

    lane = lax.broadcasted_iota(jnp.int32, (8, LANES), 1)
    at_z = {9: 10, 10: 11, 11: 9}
    at_y = {9: 10, 10: 9, 11: 11}

    def row(j, _):
        at = pl.ds(j, 8, stride=8)
        for k in range(NVAR):
            ky = at_y.get(k, k)
            fold[k, at, :] = fy[j, ky] - fy[j + 1, ky]
        return 0

    lax.fori_loop(0, 8, row, 0)

    def store(i):
        at = pl.ds(pl.multiple_of(i * 8, 8), 8)
        return pltpu.make_async_copy(out_ref.at[:, at, :], out_h.at[:, at, :], out_sem.at[i])

    def plane(i, _):
        at = pl.ds(pl.multiple_of(i * 8, 8), 8)
        to_low = lax.rem(2 * LANES - 3 - 16 * i, LANES)
        to_high = lax.rem(2 * LANES - 13 - 16 * i, LANES)
        for k in range(NVAR):
            kz = at_z.get(k, k)
            ends = fz[8, kz]
            low = pltpu.roll(ends, to_low, 1)
            high = pltpu.roll(ends, to_high, 1)
            face = jnp.where(lane < 3, low, jnp.where(lane >= 126, high, fz[i, kz]))
            after = pltpu.roll(jnp.where(lane == 0, high, face), LANES - 1, 1)
            out_ref[k, at, :] = ((face - after) + (fx[i, k] - fx[i + 1, k]) + fold[k, at, :]) * scale
        store(i).start()
        return 0

    lax.fori_loop(0, 8, plane, 0)
    for i in range(8):
        store(i).wait()


HBM = pl.BlockSpec(memory_space=pltpu.MemorySpace.HBM)
VMEM = pl.BlockSpec(memory_space=pltpu.VMEM)
PLANES = (8, LANES)
TABLES = [pltpu.SMEM((6, 32), F32), pltpu.SMEM((32,), F32), pltpu.SMEM((NS,), jnp.int32),
          pltpu.VMEM((12 * NS,) + PLANES, F32)]


def struct(*shape):
    return jax.ShapeDtypeStruct(shape, F32)


def vmem(*shape):
    return pltpu.VMEM(shape, F32)


def dma(n):
    return pltpu.SemaphoreType.DMA((n,))


def params(mib=24):
    return pltpu.CompilerParams(vmem_limit_bytes=mib << 20)


def cells(table, gas, index, u):
    halo = struct(NVAR, 24, LANES)
    return pl.pallas_call(
        cell_kernel, name="cells", in_specs=[HBM] * 4, out_specs=[VMEM] * 5,
        out_shape=[struct(256, LANES), halo, halo, halo, halo],
        scratch_shapes=TABLES + [vmem(NVAR, 64, LANES), dma(4)],
        compiler_params=params(58))(table, gas, index, u)


def own_cells(table, gas, index, kind, u):
    return pl.pallas_call(
        own_kernel, name="own_cells", in_specs=[HBM] * 5, out_specs=[VMEM] * 2,
        out_shape=[struct(12, 64, LANES), struct(NVAR + 12, 8, LANES)],
        scratch_shapes=TABLES + [pltpu.SMEM((1, 2), jnp.int32), vmem(NVAR, 64, LANES), dma(5)],
        compiler_params=params())(table, gas, index, kind, u)


def halo_cells(table, gas, index, *halos):
    return pl.pallas_call(
        halo_kernel, name="halo_cells", in_specs=[HBM] * 3 + [VMEM] * 4, out_specs=[VMEM] * 4,
        out_shape=[struct(12, 24, LANES)] * 4, scratch_shapes=TABLES + [dma(3)],
        compiler_params=params())(table, gas, index, *halos)


def rates(wide, u, coef, ends, *halos):
    flux = vmem(9, NVAR, *PLANES)
    return pl.pallas_call(
        rate_kernel, name="rates", in_specs=[VMEM] * 12, out_specs=HBM,
        out_shape=struct(NVAR, 64, LANES),
        scratch_shapes=[
            vmem(14, 30, *PLANES), vmem(14, 24, *PLANES), vmem(13, 30, *PLANES),
            vmem(9, 120, *PLANES), flux, flux, flux,
            vmem(NVAR, 64, LANES), vmem(NVAR, 64, LANES), dma(8)],
        compiler_params=params())(wide, u, coef, ends, *halos)


AXES = ("z", "yl", "x", "yh", "c")
GX = ("z", "yl")
GY = ("x", "yh", "c")


def neighbours(start, end, axis):
    up = [(i, (i + 1) % 16) for i in range(16)]
    low = lax.ppermute(end, axis, up)
    high = lax.ppermute(start, axis, [(b, a) for a, b in up])
    return low, high


def shards(preserved_vector, nasa_table, gas_constant, species_index, face_kind):
    u = preserved_vector.reshape(NVAR, 64, LANES)
    fixed = (nasa_table.T, gas_constant, species_index)
    wide, xs, xe, ys, ye = cells(*fixed, u)
    wide = lax.all_to_all(wide, AXES, 0, 0, tiled=True)
    coef, ends = own_cells(*fixed, face_kind.reshape(1, 2), u)
    halos = neighbours(xs, xe, GX) + neighbours(ys, ye, GY)
    halo_coefs = halo_cells(*fixed, *halos)
    return rates(wide, u, coef, ends, *halos, *halo_coefs).reshape(preserved_vector.shape)


def solution(mesh):
    finer = Mesh(mesh.devices.reshape(8, 2, 4, 2, 2), AXES)
    placed = (P(None, GX, GY, None), P(), P(), P(), P(GX, GY, None))
    return jax.shard_map(
        shards, mesh=finer, in_specs=placed, out_specs=P(None, GX, GY, None), check_vma=False
    )
```

```python
import jax
import jax.numpy as jnp
from jax import lax
from jax.experimental import pallas as pl
from jax.experimental.pallas import tpu as pltpu
from jax.sharding import Mesh
from jax.sharding import PartitionSpec as P


NS = 9
NVAR = 14
NEWTON = 2
EPSILON = 1e-06
COURANT = 0.8
LANES = 128
F32 = jnp.float32


def species_constants(table, gas, index, const):
    for i in range(NS):
        row = index[i]
        r = jnp.full((8, LANES), gas[row], F32)
        a = [r * jnp.full((8, LANES), table[k, row], F32) for k in range(6)]
        rest = [a[0] - r, a[1] * 0.5, a[2] * (1.0 / 3.0), a[3] * 0.25, a[4] * 0.2]
        for k, value in enumerate([r] + a + rest):
            const[12 * i + k] = value


def coefficients(u, rows):
    rho = u[0]
    for i in range(1, NS):
        rho = rho + u[i]
    inv = 1.0 / rho
    vel = [u[NS + j] * inv for j in range(3)]
    square = vel[0] * vel[0] + vel[1] * vel[1] + vel[2] * vel[2]
    target = u[NS + 3] - 0.5 * rho * square
    mix = [None] * 7
    for i in range(NS):
        for k in range(7):
            term = u[i] * rows[12 * i + k]
            mix[k] = term if mix[k] is None else mix[k] + term
    r0, a1, a2, a3, a4, a5, a6 = mix
    b1, b2, b3, b4, b5 = a1 - r0, a2 * 0.5, a3 * (1.0 / 3.0), a4 * 0.25, a5 * 0.2
    temp = jnp.ones_like(rho)
    for _ in range(NEWTON):
        energy = a6 + temp * (b1 + temp * (b2 + temp * (b3 + temp * (b4 + temp * b5))))
        slope = b1 + temp * (a2 + temp * (a3 + temp * (a4 + temp * a5)))
        temp = temp - (energy - target) / slope
    slope = b1 + temp * (a2 + temp * (a3 + temp * (a4 + temp * a5)))
    g = r0 / slope
    p = r0 * temp
    c = jnp.sqrt((1.0 + g) * p * inv)
    kinetic = 0.5 * g * square
    phi = []
    for i in range(NS):
        e = [rows[12 * i + 6 + k] for k in range(6)]
        energy = e[0] + temp * (e[1] + temp * (e[2] + temp * (e[3] + temp * (e[4] + temp * e[5]))))
        phi.append(rows[12 * i] * temp - g * energy + kinetic)
    return p, g, c, phi, vel


def halves(u, rows):
    p, g, c, phi, _ = coefficients(u, rows)
    return [0.5 * x for x in [p, g, c] + phi]


def fetch(pairs, sem):
    copies = [pltpu.make_async_copy(src, dst, sem.at[i]) for i, (src, dst) in enumerate(pairs)]
    for copy in copies:
        copy.start()
    return copies


def cell_kernel(table_h, gas_h, index_h, u_h, wide_ref, xs_ref, xe_ref, ys_ref, ye_ref,
                table, gas, index, rows, u_ref, sem):
    for copy in fetch([(table_h, table), (gas_h, gas), (index_h, index), (u_h, u_ref)], sem):
        copy.wait()
    species_constants(table, gas, index, rows)

    def body(i, fastest):
        at = pl.ds(pl.multiple_of(i * 8, 8), 8)
        u = [u_ref[k, at, :] for k in range(NVAR)]
        c, vel = coefficients(u, rows)[2::2]
        return tuple(jnp.maximum(f, jnp.abs(v) + c) for f, v in zip(fastest, vel))

    zero = jnp.zeros((8, LANES), F32)
    fastest = lax.fori_loop(0, 8, body, (zero, zero, zero), unroll=4)
    lane = lax.broadcasted_iota(jnp.int32, (8, LANES), 1)
    out = zero
    for d in range(3):
        top = jnp.max(jnp.max(fastest[d], axis=0, keepdims=True), axis=1, keepdims=True)
        out = jnp.where(lane == d, jnp.broadcast_to(top, (8, LANES)), out)
    for i in range(32):
        wide_ref[8 * i:8 * i + 8, :] = out
    for k in range(NVAR):
        xs_ref[k] = u_ref[k, 0:24, :]
        xe_ref[k] = u_ref[k, 40:64, :]
        for j in range(3):
            ys_ref[k, 8 * j:8 * j + 8, :] = u_ref[k, pl.ds(j, 8, stride=8), :]
            ye_ref[k, 8 * j:8 * j + 8, :] = u_ref[k, pl.ds(5 + j, 8, stride=8), :]


def correction(d0, d1, d2, d3):
    t0 = d0 - 1.375 * d1
    t1 = d1 - 0.625 * d2
    t2 = d3 - 1.375 * d2
    e1 = (0.609375 * d1) * d1 + 0.75 * EPSILON
    e2 = (0.609375 * d2) * d2 + 0.75 * EPSILON
    i0 = reciprocal(t0 * t0 + e1)
    i1 = reciprocal(t1 * t1 + e2)
    i2 = reciprocal(t2 * t2 + e2)
    w0 = i0 * i0
    w1 = 6.0 * (i1 * i1)
    w2 = 3.0 * (i2 * i2)
    q = 2.625 * d2
    lead = (2.25 * d1 - q) - (t0 + t0)
    return q + (w0 * lead + w1 * t1 - w2 * t2) * reciprocal(w0 + w1 + w2)


def reciprocal(x):
    return 1.0 / x


def split_fields(u, coef, order, speed):
    p, g, c, phi = coef[0], coef[1], coef[2], coef[3:]
    rho = u[0]
    for i in range(1, NS):
        rho = rho + u[i]
    inv = 0.5 / rho
    vel = [u[NS + j] * inv for j in order]
    plus, minus = vel[0] + speed, vel[0] - speed
    rows = u[:NS] + [u[NS + j] for j in order] + [u[NS + 3], u[NS + 4], rho]
    up = [x * plus for x in rows]
    down = [x * minus for x in rows]
    work = (p + p) * vel[0]
    for side in (up, down):
        side[NS] = side[NS] + p
        side[NS + 3] = side[NS + 3] + work
    mean = [x * inv for x in u[:NS]] + vel + [u[NS + 4] * inv, g, c] + phi
    return up, down, mean


def face_flux(left, right, jump, put):
    def mean(k):
        return left(k) + right(k)

    g, c = mean(13), mean(14)
    vel = [mean(9 + k) for k in range(3)]
    ig = 1.0 / g
    ic = 1.0 / c
    inv = ic * ic
    ihc = 0.5 * ic
    gs = g * inv
    gu = [gs * v for v in vel]
    square = vel[0] * vel[0] + vel[1] * vel[1] + vel[2] * vel[2]
    dot = None
    phis = []
    for k in range(NS):
        phi = mean(15 + k)
        term = mean(k) * phi
        dot = term if dot is None else dot + term
        phis.append(phi * inv)
    h = (c * c - dot) * ig + square
    pressure, swings, sums = {}, {}, {}
    for side in range(2):
        for i in range(side, 4 + side):
            dp = phis[0] * jump(side, i, 0)
            for k in range(1, NS):
                dp = dp + phis[k] * jump(side, i, k)
            v = [jump(side, i, NS + k) for k in range(3)]
            s = jump(side, i, 14)
            dp = dp + (gs * jump(side, i, 12) - (gu[0] * v[0] + gu[1] * v[1] + gu[2] * v[2]))
            pressure[side, i] = dp
            swings[side, i] = (v[0] - vel[0] * s) * ihc
            sums[side, i] = s

    def amplitude(wave):
        p = [wave(0, i) for i in range(4)]
        m = [wave(1, i) for i in range(4, 0, -1)]
        return correction(*p) - correction(*m)

    slower = amplitude(lambda side, i: 0.5 * pressure[side, i] - swings[side, i])
    faster = amplitude(lambda side, i: 0.5 * pressure[side, i] + swings[side, i])
    first = amplitude(lambda side, i: jump(side, i, 10) - vel[1] * sums[side, i])
    second = amplitude(lambda side, i: jump(side, i, 11) - vel[2] * sums[side, i])
    acoustic = slower + faster
    swing = (faster - slower) * c
    energy = h * acoustic + vel[0] * swing + vel[1] * first + vel[2] * second
    z = mean(12)
    put(13, z * acoustic + amplitude(lambda side, i: jump(side, i, 13) - z * pressure[side, i]))
    total = dot = None
    for k in range(NS):
        yk = mean(k)
        species = amplitude(lambda side, i: jump(side, i, k) - yk * pressure[side, i])
        put(k, yk * acoustic + species)
        term = phis[k] * species
        total = species if total is None else total + species
        dot = term if dot is None else dot + term
    both = acoustic + total
    put(9, vel[0] * both + swing)
    put(10, vel[1] * both + first)
    put(11, vel[2] * both + second)
    put(12, energy + square * total - (dot * (c * c)) * ig)


def own_kernel(table_h, gas_h, index_h, kind_h, u_h, coef_ref, ends_ref,
               table, gas, index, rows, kind, u_ref, sem):
    for copy in fetch([(table_h, table), (gas_h, gas), (index_h, index), (kind_h, kind),
                       (u_h, u_ref)], sem):
        copy.wait()
    species_constants(table, gas, index, rows)
    lane = lax.broadcasted_iota(jnp.int32, (8, LANES), 1)
    slot = lane % 16
    group = lane // 16
    low_wall = kind[0, 0] == 1
    high_wall = kind[0, 1] == 1

    def pick(k):
        packed = jnp.zeros((8, LANES), F32)
        for plane in range(8):
            v = u_ref[k, 8 * plane:8 * plane + 8, :]
            low = pltpu.roll(v, (16 * plane + 3) % LANES, 1)
            high = pltpu.roll(v, (16 * plane + 8 - 123) % LANES, 1)
            packed = jnp.where(group == plane, jnp.where(slot < 8, low, high), packed)

        def at(shift):
            return pltpu.roll(packed, shift % LANES, 1)

        sign = -1.0 if k == NS + 2 else 1.0
        mirror = jnp.where(slot == 2, at(-1), jnp.where(slot == 1, at(-3), at(-5))) * sign
        copy = jnp.where(slot == 2, at(-1), jnp.where(slot == 1, at(-2), at(-3)))
        low = jnp.where(low_wall, mirror, copy)
        mirror = jnp.where(slot == 13, at(1), jnp.where(slot == 14, at(3), at(5))) * sign
        copy = jnp.where(slot == 13, at(1), jnp.where(slot == 14, at(2), at(3)))
        high = jnp.where(high_wall, mirror, copy)
        ends_ref[k] = jnp.where(slot < 3, low, jnp.where(slot > 12, high, packed))
        return 0

    for k in range(NVAR):
        pick(k)
    for k, value in enumerate(halves([ends_ref[k] for k in range(NVAR)], rows)):
        ends_ref[NVAR + k] = value

    def plane(i, _):
        at = pl.ds(pl.multiple_of(i * 8, 8), 8)
        for k, value in enumerate(halves([u_ref[k, at, :] for k in range(NVAR)], rows)):
            coef_ref[k, at, :] = value
        return 0

    lax.fori_loop(0, 8, plane, 0, unroll=4)


def halo_kernel(table_h, gas_h, index_h, *refs):
    halos, outs, (table, gas, index, rows, sem) = refs[:4], refs[4:8], refs[8:]
    for copy in fetch([(table_h, table), (gas_h, gas), (index_h, index)], sem):
        copy.wait()
    species_constants(table, gas, index, rows)
    for u_ref, out_ref in zip(halos, outs):
        def plane(i, _, u_ref=u_ref, out_ref=out_ref):
            at = pl.ds(pl.multiple_of(i * 8, 8), 8)
            for k, value in enumerate(halves([u_ref[k, at, :] for k in range(NVAR)], rows)):
                out_ref[k, at, :] = value
            return 0

        lax.fori_loop(0, 3, plane, 0, unroll=True)


def emit(flux, f, base):
    def put(k, value):
        flux[f, k] = value * (1.0 / 6.0) + base(k)

    return put


def column_kernel(wide, u_ref, coef_ref, ends_ref, out_ref, speed_ref, pm, mean, columns, fz):
    top = wide[0:8, :]
    for i in range(1, 32):
        top = jnp.maximum(top, wide[8 * i:8 * i + 8, :])
    top = jnp.max(top, axis=0, keepdims=True)
    lane = lax.broadcasted_iota(jnp.int32, (1, LANES), 1)
    speeds = []
    for d in range(3):
        one = jnp.max(jnp.where(lane == d, top, 0.0), axis=1, keepdims=True)
        speeds.append(jnp.broadcast_to(0.5 * one, (8, LANES)))
    for d in range(3):
        speed_ref[d] = speeds[d]
    speed_ref[3] = (0.5 * COURANT) / (speeds[0] + speeds[1] + speeds[2])

    def column(f, u, coef):
        up, down, m = split_fields(u, coef, (2, 0, 1), speeds[2])
        for k in range(24):
            mean[f, k] = m[k] + pltpu.roll(m[k], 1, 1)
        for k in range(15):
            before = pltpu.roll(up[k], 1, 1)
            step = up[k] - before
            for i, shift in enumerate((2, 1, 0, LANES - 1)):
                columns[f, 15 * i + k] = pltpu.roll(step, shift, 1) if shift else step
            pm[f, k] = before + down[k]
            step = down[k] - pltpu.roll(down[k], 1, 1)
            for i, shift in enumerate((1, 0, LANES - 1, LANES - 2)):
                columns[f, 60 + 15 * i + k] = pltpu.roll(step, shift, 1) if shift else step

    column(8, [ends_ref[k] for k in range(NVAR)], [ends_ref[NVAR + k] for k in range(12)])

    def plane(i, _):
        at = pl.ds(pl.multiple_of(i * 8, 8), 8)
        column(i, [u_ref[k, at, :] for k in range(NVAR)], [coef_ref[k, at, :] for k in range(12)])
        return 0

    lax.fori_loop(0, 8, plane, 0)

    def upright(f, _):
        face_flux(lambda k: mean[f, k], lambda k: 0.0,
                  lambda side, i, k: columns[f, 60 * side + 15 * (i - side) + k],
                  emit(fz, f, lambda k: pm[f, k]))
        return 0

    lax.fori_loop(0, 9, upright, 0)
    lane = lax.broadcasted_iota(jnp.int32, (8, LANES), 1)
    at_z = {9: 10, 10: 11, 11: 9}

    def merge(i, _):
        at = pl.ds(pl.multiple_of(i * 8, 8), 8)
        to_low = lax.rem(2 * LANES - 3 - 16 * i, LANES)
        to_high = lax.rem(2 * LANES - 13 - 16 * i, LANES)
        for k in range(NVAR):
            kz = at_z.get(k, k)
            ends = fz[8, kz]
            low = pltpu.roll(ends, to_low, 1)
            high = pltpu.roll(ends, to_high, 1)
            face = jnp.where(lane < 3, low, jnp.where(lane >= 126, high, fz[i, kz]))
            after = pltpu.roll(jnp.where(lane == 0, high, face), LANES - 1, 1)
            out_ref[k, at, :] = face - after
        return 0

    lax.fori_loop(0, 8, merge, 0)


def rate_kernel(speed_ref, u_ref, coef_ref, z_ref, *refs):
    halo_u, halo_c, out_h = refs[:4], refs[4:8], refs[8]
    (pm, mean, jumps, fx, fy, fold, out_ref, out_sem) = refs[9:]
    speeds = [speed_ref[d] for d in range(2)]
    scale = speed_ref[3]
    for d, order, strided, flux in ((0, (0, 1, 2), False, fx), (1, (1, 0, 2), True, fy)):
        def cell(i, u, coef, d=d, order=order):
            up, down, m = split_fields(u, coef, order, speeds[d])
            for k in range(24):
                mean[i, k] = m[k]
            for k in range(15):
                pm[i, k] = up[k]
                pm[i, 15 + k] = down[k]

        def own(i, _, cell=cell, strided=strided):
            at = pl.ds(i, 8, stride=8) if strided else pl.ds(pl.multiple_of(i * 8, 8), 8)
            cell(i + 3, [u_ref[k, at, :] for k in range(NVAR)],
                 [coef_ref[k, at, :] for k in range(12)])
            return 0

        lax.fori_loop(0, 8, own, 0, unroll=2)

        for high in range(2):
            def halo(i, _, cell=cell, d=d, high=high):
                at = pl.ds(pl.multiple_of(i * 8, 8), 8)
                cell(i + 11 * high, [halo_u[2 * d + high][k, at, :] for k in range(NVAR)],
                     [halo_c[2 * d + high][k, at, :] for k in range(12)])
                return 0

            lax.fori_loop(0, 3, halo, 0, unroll=True)

        def jump(i, _):
            for k in range(30):
                jumps[i, k] = pm[i + 1, k] - pm[i, k]
            return 0

        lax.fori_loop(0, 13, jump, 0, unroll=True)

        def face(f, _, flux=flux):
            face_flux(lambda k: mean[f + 2, k], lambda k: mean[f + 3, k],
                      lambda side, i, k: jumps[f + i, 15 * side + k],
                      emit(flux, f, lambda k: pm[f + 2, k] + pm[f + 3, 15 + k]))
            return 0

        lax.fori_loop(0, 9, face, 0)

    at_y = {9: 10, 10: 9, 11: 11}

    def row(j, _):
        at = pl.ds(j, 8, stride=8)
        for k in range(NVAR):
            ky = at_y.get(k, k)
            fold[k, at, :] = fy[j, ky] - fy[j + 1, ky]
        return 0

    lax.fori_loop(0, 8, row, 0)

    def store(i):
        at = pl.ds(pl.multiple_of(i * 8, 8), 8)
        return pltpu.make_async_copy(out_ref.at[:, at, :], out_h.at[:, at, :], out_sem.at[i])

    def plane(i, _):
        at = pl.ds(pl.multiple_of(i * 8, 8), 8)
        for k in range(NVAR):
            out_ref[k, at, :] = (z_ref[k, at, :] + (fx[i, k] - fx[i + 1, k]) + fold[k, at, :]) * scale
        store(i).start()
        return 0

    lax.fori_loop(0, 8, plane, 0)
    for i in range(8):
        store(i).wait()


HBM = pl.BlockSpec(memory_space=pltpu.MemorySpace.HBM)
VMEM = pl.BlockSpec(memory_space=pltpu.VMEM)
PLANES = (8, LANES)
TABLES = [pltpu.SMEM((6, 32), F32), pltpu.SMEM((32,), F32), pltpu.SMEM((NS,), jnp.int32),
          pltpu.VMEM((12 * NS,) + PLANES, F32)]


def struct(*shape):
    return jax.ShapeDtypeStruct(shape, F32)


def vmem(*shape):
    return pltpu.VMEM(shape, F32)


def dma(n):
    return pltpu.SemaphoreType.DMA((n,))


def params(mib=20):
    return pltpu.CompilerParams(vmem_limit_bytes=mib << 20)


def cells(table, gas, index, u):
    halo = struct(NVAR, 24, LANES)
    return pl.pallas_call(
        cell_kernel, name="cells", in_specs=[HBM] * 4, out_specs=[VMEM] * 5,
        out_shape=[struct(256, LANES), halo, halo, halo, halo],
        scratch_shapes=TABLES + [vmem(NVAR, 64, LANES), dma(4)],
        compiler_params=params(58))(table, gas, index, u)


def own_cells(table, gas, index, kind, u):
    return pl.pallas_call(
        own_kernel, name="own_cells", in_specs=[HBM] * 5, out_specs=[VMEM] * 2,
        out_shape=[struct(12, 64, LANES), struct(NVAR + 12, 8, LANES)],
        scratch_shapes=TABLES + [pltpu.SMEM((1, 2), jnp.int32), vmem(NVAR, 64, LANES), dma(5)],
        compiler_params=params())(table, gas, index, kind, u)


def halo_cells(table, gas, index, *halos):
    return pl.pallas_call(
        halo_kernel, name="halo_cells", in_specs=[HBM] * 3 + [VMEM] * 4, out_specs=[VMEM] * 4,
        out_shape=[struct(12, 24, LANES)] * 4, scratch_shapes=TABLES + [dma(3)],
        compiler_params=params())(table, gas, index, *halos)


def columns(wide, u, coef, ends):
    return pl.pallas_call(
        column_kernel, name="columns", in_specs=[VMEM] * 4, out_specs=[VMEM] * 2,
        out_shape=[struct(NVAR, 64, LANES), struct(4, 8, LANES)],
        scratch_shapes=[vmem(9, 15, *PLANES), vmem(9, 24, *PLANES), vmem(9, 120, *PLANES),
                        vmem(9, NVAR, *PLANES)],
        compiler_params=params())(wide, u, coef, ends)


def rates(speed, u, coef, z, *halos):
    flux = vmem(9, NVAR, *PLANES)
    return pl.pallas_call(
        rate_kernel, name="rates", in_specs=[VMEM] * 12, out_specs=HBM,
        out_shape=struct(NVAR, 64, LANES),
        scratch_shapes=[
            vmem(14, 30, *PLANES), vmem(14, 24, *PLANES), vmem(13, 30, *PLANES), flux, flux,
            vmem(NVAR, 64, LANES), vmem(NVAR, 64, LANES), dma(8)],
        compiler_params=params())(speed, u, coef, z, *halos)


AXES = ("z", "yl", "x", "yh", "c")
GX = ("z", "yl")
GY = ("x", "yh", "c")


def neighbours(start, end, axis):
    up = [(i, (i + 1) % 16) for i in range(16)]
    low = lax.ppermute(end, axis, up)
    high = lax.ppermute(start, axis, [(b, a) for a, b in up])
    return low, high


def shards(preserved_vector, nasa_table, gas_constant, species_index, face_kind):
    u = preserved_vector.reshape(NVAR, 64, LANES)
    fixed = (nasa_table.T, gas_constant, species_index)
    wide, xs, xe, ys, ye = cells(*fixed, u)
    wide = lax.all_to_all(wide, AXES, 0, 0, tiled=True)
    coef, ends = own_cells(*fixed, face_kind.reshape(1, 2), u)
    halos = neighbours(xs, xe, GX) + neighbours(ys, ye, GY)
    z, speed = columns(wide, u, coef, ends)
    halo_coefs = halo_cells(*fixed, *halos)
    return rates(speed, u, coef, z, *halos, *halo_coefs).reshape(preserved_vector.shape)


def solution(mesh):
    finer = Mesh(mesh.devices.reshape(8, 2, 4, 2, 2), AXES)
    placed = (P(None, GX, GY, None), P(), P(), P(), P(GX, GY, None))
    return jax.shard_map(
        shards, mesh=finer, in_specs=placed, out_specs=P(None, GX, GY, None), check_vma=False
    )
```

```python
import jax
import jax.numpy as jnp
from jax import lax
from jax.experimental import pallas as pl
from jax.experimental.pallas import tpu as pltpu
from jax.sharding import Mesh
from jax.sharding import PartitionSpec as P


NS = 9
NVAR = 14
NEWTON = 2
EPSILON = 1e-06
COURANT = 0.8
LANES = 128
F32 = jnp.float32


def species_constants(table, gas, index, const):
    for i in range(NS):
        row = index[i]
        r = jnp.full((8, LANES), gas[row], F32)
        a = [r * jnp.full((8, LANES), table[k, row], F32) for k in range(6)]
        rest = [a[0] - r, a[1] * 0.5, a[2] * (1.0 / 3.0), a[3] * 0.25, a[4] * 0.2]
        for k, value in enumerate([r] + a + rest):
            const[12 * i + k] = value


def coefficients(u, rows):
    rho = u[0]
    for i in range(1, NS):
        rho = rho + u[i]
    inv = 1.0 / rho
    vel = [u[NS + j] * inv for j in range(3)]
    square = vel[0] * vel[0] + vel[1] * vel[1] + vel[2] * vel[2]
    target = u[NS + 3] - 0.5 * rho * square
    mix = [None] * 7
    for i in range(NS):
        for k in range(7):
            term = u[i] * rows[12 * i + k]
            mix[k] = term if mix[k] is None else mix[k] + term
    r0, a1, a2, a3, a4, a5, a6 = mix
    b1, b2, b3, b4, b5 = a1 - r0, a2 * 0.5, a3 * (1.0 / 3.0), a4 * 0.25, a5 * 0.2
    temp = jnp.ones_like(rho)
    for _ in range(NEWTON):
        energy = a6 + temp * (b1 + temp * (b2 + temp * (b3 + temp * (b4 + temp * b5))))
        slope = b1 + temp * (a2 + temp * (a3 + temp * (a4 + temp * a5)))
        temp = temp - (energy - target) / slope
    slope = b1 + temp * (a2 + temp * (a3 + temp * (a4 + temp * a5)))
    g = r0 / slope
    p = r0 * temp
    c = jnp.sqrt((1.0 + g) * p * inv)
    kinetic = 0.5 * g * square
    phi = []
    for i in range(NS):
        e = [rows[12 * i + 6 + k] for k in range(6)]
        energy = e[0] + temp * (e[1] + temp * (e[2] + temp * (e[3] + temp * (e[4] + temp * e[5]))))
        phi.append(rows[12 * i] * temp - g * energy + kinetic)
    return p, g, c, phi, vel


def halves(u, rows):
    p, g, c, phi, _ = coefficients(u, rows)
    return [0.5 * x for x in [p, g, c] + phi]


def fetch(pairs, sem):
    copies = [pltpu.make_async_copy(src, dst, sem.at[i]) for i, (src, dst) in enumerate(pairs)]
    for copy in copies:
        copy.start()
    return copies


def cell_kernel(table_h, gas_h, index_h, u_h, wide_ref, xs_ref, xe_ref, ys_ref, ye_ref,
                table, gas, index, rows, u_ref, sem):
    for copy in fetch([(table_h, table), (gas_h, gas), (index_h, index), (u_h, u_ref)], sem):
        copy.wait()
    species_constants(table, gas, index, rows)

    def body(i, fastest):
        at = pl.ds(pl.multiple_of(i * 8, 8), 8)
        u = [u_ref[k, at, :] for k in range(NVAR)]
        c, vel = coefficients(u, rows)[2::2]
        return tuple(jnp.maximum(f, jnp.abs(v) + c) for f, v in zip(fastest, vel))

    zero = jnp.zeros((8, LANES), F32)
    fastest = lax.fori_loop(0, 8, body, (zero, zero, zero), unroll=4)
    lane = lax.broadcasted_iota(jnp.int32, (8, LANES), 1)
    out = zero
    for d in range(3):
        top = jnp.max(jnp.max(fastest[d], axis=0, keepdims=True), axis=1, keepdims=True)
        out = jnp.where(lane == d, jnp.broadcast_to(top, (8, LANES)), out)
    for i in range(32):
        wide_ref[8 * i:8 * i + 8, :] = out
    for k in range(NVAR):
        xs_ref[k] = u_ref[k, 0:24, :]
        xe_ref[k] = u_ref[k, 40:64, :]
        for j in range(3):
            ys_ref[k, 8 * j:8 * j + 8, :] = u_ref[k, pl.ds(j, 8, stride=8), :]
            ye_ref[k, 8 * j:8 * j + 8, :] = u_ref[k, pl.ds(5 + j, 8, stride=8), :]


def correction(d0, d1, d2, d3):
    t0 = d0 - 1.375 * d1
    t1 = d1 - 0.625 * d2
    t2 = d3 - 1.375 * d2
    e1 = (0.609375 * d1) * d1 + 0.75 * EPSILON
    e2 = (0.609375 * d2) * d2 + 0.75 * EPSILON
    i0 = reciprocal(t0 * t0 + e1)
    i1 = reciprocal(t1 * t1 + e2)
    i2 = reciprocal(t2 * t2 + e2)
    w0 = i0 * i0
    w1 = 6.0 * (i1 * i1)
    w2 = 3.0 * (i2 * i2)
    q = 2.625 * d2
    lead = (2.25 * d1 - q) - (t0 + t0)
    return q + (w0 * lead + w1 * t1 - w2 * t2) * reciprocal(w0 + w1 + w2)


def reciprocal(x):
    return 1.0 / x


def split_fields(u, coef, order, speed):
    p, g, c, phi = coef[0], coef[1], coef[2], coef[3:]
    rho = u[0]
    for i in range(1, NS):
        rho = rho + u[i]
    inv = 0.5 / rho
    vel = [u[NS + j] * inv for j in order]
    plus, minus = vel[0] + speed, vel[0] - speed
    rows = u[:NS] + [u[NS + j] for j in order] + [u[NS + 3], u[NS + 4], rho]
    up = [x * plus for x in rows]
    down = [x * minus for x in rows]
    work = (p + p) * vel[0]
    for side in (up, down):
        side[NS] = side[NS] + p
        side[NS + 3] = side[NS + 3] + work
    mean = [x * inv for x in u[:NS]] + vel + [u[NS + 4] * inv, g, c] + phi
    return up, down, mean


def face_flux(left, right, jump, put):
    def mean(k):
        return left(k) + right(k)

    g, c = mean(13), mean(14)
    vel = [mean(9 + k) for k in range(3)]
    ig = 1.0 / g
    ic = 1.0 / c
    inv = ic * ic
    ihc = 0.5 * ic
    gs = g * inv
    gu = [gs * v for v in vel]
    square = vel[0] * vel[0] + vel[1] * vel[1] + vel[2] * vel[2]
    dot = None
    phis = []
    for k in range(NS):
        phi = mean(15 + k)
        term = mean(k) * phi
        dot = term if dot is None else dot + term
        phis.append(phi * inv)
    h = (c * c - dot) * ig + square
    pressure, swings, sums = {}, {}, {}
    for side in range(2):
        for i in range(side, 4 + side):
            dp = phis[0] * jump(side, i, 0)
            for k in range(1, NS):
                dp = dp + phis[k] * jump(side, i, k)
            v = [jump(side, i, NS + k) for k in range(3)]
            s = jump(side, i, 14)
            dp = dp + (gs * jump(side, i, 12) - (gu[0] * v[0] + gu[1] * v[1] + gu[2] * v[2]))
            pressure[side, i] = dp
            swings[side, i] = (v[0] - vel[0] * s) * ihc
            sums[side, i] = s

    def amplitude(wave):
        p = [wave(0, i) for i in range(4)]
        m = [wave(1, i) for i in range(4, 0, -1)]
        return correction(*p) - correction(*m)

    slower = amplitude(lambda side, i: 0.5 * pressure[side, i] - swings[side, i])
    faster = amplitude(lambda side, i: 0.5 * pressure[side, i] + swings[side, i])
    first = amplitude(lambda side, i: jump(side, i, 10) - vel[1] * sums[side, i])
    second = amplitude(lambda side, i: jump(side, i, 11) - vel[2] * sums[side, i])
    acoustic = slower + faster
    swing = (faster - slower) * c
    energy = h * acoustic + vel[0] * swing + vel[1] * first + vel[2] * second
    z = mean(12)
    put(13, z * acoustic + amplitude(lambda side, i: jump(side, i, 13) - z * pressure[side, i]))
    total = dot = None
    for k in range(NS):
        yk = mean(k)
        species = amplitude(lambda side, i: jump(side, i, k) - yk * pressure[side, i])
        put(k, yk * acoustic + species)
        term = phis[k] * species
        total = species if total is None else total + species
        dot = term if dot is None else dot + term
    both = acoustic + total
    put(9, vel[0] * both + swing)
    put(10, vel[1] * both + first)
    put(11, vel[2] * both + second)
    put(12, energy + square * total - (dot * (c * c)) * ig)


def own_kernel(table_h, gas_h, index_h, kind_h, u_ref, coef_ref, tall_ref, tall_coef, const_ref,
               table, gas, index, rows, kind, turned, sem):
    copies = fetch([(kind_h, kind), (table_h, table), (gas_h, gas), (index_h, index)], sem)
    copies[0].wait()
    sub = lax.broadcasted_iota(jnp.int32, (8, LANES), 0)
    lane = lax.broadcasted_iota(jnp.int32, (8, LANES), 1)
    left = lane < 64
    low_wall = kind[0, 0] == 1
    high_wall = kind[0, 1] == 1
    for pair in range(NVAR // 2):
        turned[pair] = jnp.concatenate([u_ref[2 * pair], u_ref[2 * pair + 1]], axis=0).T
    for k in range(NVAR):
        pair, second = divmod(k, 2)
        for b in range(8):
            top = turned[pair, pl.ds(b, 8, stride=8), :]
            bottom = turned[pair, pl.ds(64 + b, 8, stride=8), :]
            if second:
                tall_ref[k, b + 3] = jnp.where(left, pltpu.roll(top, 64, 1), bottom)
            else:
                tall_ref[k, b + 3] = jnp.where(left, top, pltpu.roll(bottom, 64, 1))
        sign = -1.0 if k == NS + 2 else 1.0
        for ghost in range(3):
            down = pltpu.roll(tall_ref[k, 10 - ghost], 1, 0)
            edge = jnp.where(low_wall, tall_ref[k, 3 + ghost] * sign, tall_ref[k, 3])
            edge = jnp.where(left, edge, pltpu.roll(down, 64, 1))
            tall_ref[k, 2 - ghost] = jnp.where(sub == 0, edge, down)
            up = pltpu.roll(tall_ref[k, 3 + ghost], 7, 0)
            edge = jnp.where(high_wall, tall_ref[k, 10 - ghost] * sign, tall_ref[k, 10])
            edge = jnp.where(left, pltpu.roll(up, 64, 1), edge)
            tall_ref[k, 11 + ghost] = jnp.where(sub == 7, edge, up)
    for copy in copies[1:]:
        copy.wait()
    species_constants(table, gas, index, rows)
    for k in range(12 * NS):
        const_ref[k] = rows[k, 0:1, :]

    def plane(i, _):
        at = pl.ds(pl.multiple_of(i * 8, 8), 8)
        for k, value in enumerate(halves([u_ref[k, at, :] for k in range(NVAR)], rows)):
            coef_ref[k, at, :] = value
        return 0

    lax.fori_loop(0, 8, plane, 0, unroll=4)

    def tall(i, _):
        for k, value in enumerate(halves([tall_ref[k, i] for k in range(NVAR)], rows)):
            tall_coef[k, i] = value
        return 0

    lax.fori_loop(0, 14, tall, 0, unroll=4 if 14 % 4 == 0 else 2)


def emit(flux, f, base):
    def put(k, value):
        flux[f, k] = value * (1.0 / 6.0) + base(k)

    return put


def column_kernel(wide, tall_ref, tall_coef, out_ref, speed_ref, pm, mean, jumps, fz, turned):
    top = wide[0:8, :]
    for i in range(1, 32):
        top = jnp.maximum(top, wide[8 * i:8 * i + 8, :])
    top = jnp.max(top, axis=0, keepdims=True)
    lane = lax.broadcasted_iota(jnp.int32, (1, LANES), 1)
    speeds = []
    for d in range(3):
        one = jnp.max(jnp.where(lane == d, top, 0.0), axis=1, keepdims=True)
        speeds.append(jnp.broadcast_to(0.5 * one, (8, LANES)))
    for d in range(3):
        speed_ref[d] = speeds[d]
    speed_ref[3] = (0.5 * COURANT) / (speeds[0] + speeds[1] + speeds[2])

    def cell(i, _):
        up, down, m = split_fields([tall_ref[k, i] for k in range(NVAR)],
                                   [tall_coef[k, i] for k in range(12)], (2, 0, 1), speeds[2])
        for k in range(24):
            mean[i, k] = m[k]
        for k in range(15):
            pm[i, k] = up[k]
            pm[i, 15 + k] = down[k]
        return 0

    lax.fori_loop(0, 14, cell, 0, unroll=2)

    def jump(i, _):
        for k in range(30):
            jumps[i, k] = pm[i + 1, k] - pm[i, k]
        return 0

    lax.fori_loop(0, 13, jump, 0, unroll=True)

    def face(f, _):
        face_flux(lambda k: mean[f + 2, k], lambda k: mean[f + 3, k],
                  lambda side, i, k: jumps[f + i, 15 * side + k],
                  emit(fz, f, lambda k: pm[f + 2, k] + pm[f + 3, 15 + k]))
        return 0

    lax.fori_loop(0, 9, face, 0)
    left = lax.broadcasted_iota(jnp.int32, (8, LANES), 1) < 64
    at_z = {9: 10, 10: 11, 11: 9}
    for pair in range(NVAR // 2):
        first, second = [at_z.get(k, k) for k in (2 * pair, 2 * pair + 1)]
        for b in range(8):
            x = fz[b, first] - fz[b + 1, first]
            y = fz[b, second] - fz[b + 1, second]
            turned[pair, pl.ds(b, 8, stride=8), :] = jnp.where(left, x, pltpu.roll(y, 64, 1))
            turned[pair, pl.ds(64 + b, 8, stride=8), :] = jnp.where(left, pltpu.roll(x, 64, 1), y)
    for pair in range(NVAR // 2):
        back = turned[pair].T
        out_ref[2 * pair] = back[0:64]
        out_ref[2 * pair + 1] = back[64:128]


def rate_kernel(speed_ref, u_ref, coef_ref, z_ref, const, *refs):
    halo_u, out_h = refs[:4], refs[4]
    (pm, mean, jumps, fx, fy, fold, out_ref, out_sem) = refs[5:]
    speeds = [speed_ref[d] for d in range(2)]
    scale = speed_ref[3]
    for d, order, strided, flux in ((0, (0, 1, 2), False, fx), (1, (1, 0, 2), True, fy)):
        def cell(i, u, coef, d=d, order=order):
            up, down, m = split_fields(u, coef, order, speeds[d])
            for k in range(24):
                mean[i, k] = m[k]
            for k in range(15):
                pm[i, k] = up[k]
                pm[i, 15 + k] = down[k]

        def own(i, _, cell=cell, strided=strided):
            at = pl.ds(i, 8, stride=8) if strided else pl.ds(pl.multiple_of(i * 8, 8), 8)
            cell(i + 3, [u_ref[k, at, :] for k in range(NVAR)],
                 [coef_ref[k, at, :] for k in range(12)])
            return 0

        lax.fori_loop(0, 8, own, 0, unroll=2)

        for high in range(2):
            def halo(i, _, cell=cell, d=d, high=high):
                at = pl.ds(pl.multiple_of(i * 8, 8), 8)
                u = [halo_u[2 * d + high][k, at, :] for k in range(NVAR)]
                cell(i + 11 * high, u, halves(u, const))
                return 0

            lax.fori_loop(0, 3, halo, 0, unroll=True)

        def jump(i, _):
            for k in range(30):
                jumps[i, k] = pm[i + 1, k] - pm[i, k]
            return 0

        lax.fori_loop(0, 13, jump, 0, unroll=True)

        def face(f, _, flux=flux):
            face_flux(lambda k: mean[f + 2, k], lambda k: mean[f + 3, k],
                      lambda side, i, k: jumps[f + i, 15 * side + k],
                      emit(flux, f, lambda k: pm[f + 2, k] + pm[f + 3, 15 + k]))
            return 0

        lax.fori_loop(0, 9, face, 0)

    at_y = {9: 10, 10: 9, 11: 11}

    def row(j, _):
        at = pl.ds(j, 8, stride=8)
        for k in range(NVAR):
            ky = at_y.get(k, k)
            fold[k, at, :] = fy[j, ky] - fy[j + 1, ky]
        return 0

    lax.fori_loop(0, 8, row, 0)

    def store(i):
        at = pl.ds(pl.multiple_of(i * 8, 8), 8)
        return pltpu.make_async_copy(out_ref.at[:, at, :], out_h.at[:, at, :], out_sem.at[i])

    def plane(i, _):
        at = pl.ds(pl.multiple_of(i * 8, 8), 8)
        for k in range(NVAR):
            out_ref[k, at, :] = (z_ref[k, at, :] + (fx[i, k] - fx[i + 1, k]) + fold[k, at, :]) * scale
        store(i).start()
        return 0

    lax.fori_loop(0, 8, plane, 0)
    for i in range(8):
        store(i).wait()


HBM = pl.BlockSpec(memory_space=pltpu.MemorySpace.HBM)
VMEM = pl.BlockSpec(memory_space=pltpu.VMEM)
PLANES = (8, LANES)
TABLES = [pltpu.SMEM((6, 32), F32), pltpu.SMEM((32,), F32), pltpu.SMEM((NS,), jnp.int32),
          pltpu.VMEM((12 * NS,) + PLANES, F32)]


def struct(*shape):
    return jax.ShapeDtypeStruct(shape, F32)


def vmem(*shape):
    return pltpu.VMEM(shape, F32)


def dma(n):
    return pltpu.SemaphoreType.DMA((n,))


def params(mib=20):
    return pltpu.CompilerParams(vmem_limit_bytes=mib << 20)


def cells(table, gas, index, u):
    halo = struct(NVAR, 24, LANES)
    return pl.pallas_call(
        cell_kernel, name="cells", in_specs=[HBM] * 4, out_specs=[VMEM] * 5,
        out_shape=[struct(256, LANES), halo, halo, halo, halo],
        scratch_shapes=TABLES + [vmem(NVAR, 64, LANES), dma(4)],
        compiler_params=params(58))(table, gas, index, u)


def own_cells(table, gas, index, kind, u):
    return pl.pallas_call(
        own_kernel, name="own_cells", in_specs=[HBM] * 4 + [VMEM], out_specs=[VMEM] * 4,
        out_shape=[struct(12, 64, LANES), struct(NVAR, 14, 8, LANES), struct(12, 14, 8, LANES),
                   struct(12 * NS, 1, LANES)],
        scratch_shapes=TABLES + [pltpu.SMEM((1, 2), jnp.int32),
                                     vmem(NVAR // 2, LANES, LANES), dma(4)],
        compiler_params=params())(table, gas, index, kind, u)


def columns(wide, tall, tall_coef):
    return pl.pallas_call(
        column_kernel, name="columns", in_specs=[VMEM] * 3, out_specs=[VMEM] * 2,
        out_shape=[struct(NVAR, 64, LANES), struct(4, 8, LANES)],
        scratch_shapes=[vmem(14, 30, *PLANES), vmem(14, 24, *PLANES), vmem(13, 30, *PLANES),
                        vmem(9, NVAR, *PLANES), vmem(NVAR // 2, LANES, LANES)],
        compiler_params=params())(wide, tall, tall_coef)


def rates(speed, u, coef, z, const, *halos):
    flux = vmem(9, NVAR, *PLANES)
    return pl.pallas_call(
        rate_kernel, name="rates", in_specs=[VMEM] * 9, out_specs=HBM,
        out_shape=struct(NVAR, 64, LANES),
        scratch_shapes=[
            vmem(14, 30, *PLANES), vmem(14, 24, *PLANES), vmem(13, 30, *PLANES), flux, flux,
            vmem(NVAR, 64, LANES), vmem(NVAR, 64, LANES), dma(8)],
        compiler_params=params())(speed, u, coef, z, const, *halos)


AXES = ("z", "yl", "x", "yh", "c")
GX = ("z", "yl")
GY = ("x", "yh", "c")


def neighbours(start, end, axis):
    up = [(i, (i + 1) % 16) for i in range(16)]
    low = lax.ppermute(end, axis, up)
    high = lax.ppermute(start, axis, [(b, a) for a, b in up])
    return low, high


def shards(preserved_vector, nasa_table, gas_constant, species_index, face_kind):
    u = preserved_vector.reshape(NVAR, 64, LANES)
    fixed = (nasa_table.T, gas_constant, species_index)
    wide, xs, xe, ys, ye = cells(*fixed, u)
    wide = lax.all_to_all(wide, AXES, 0, 0, tiled=True)
    coef, tall, tall_coef, const = own_cells(*fixed, face_kind.reshape(1, 2), u)
    halos = neighbours(xs, xe, GX) + neighbours(ys, ye, GY)
    z, speed = columns(wide, tall, tall_coef)
    return rates(speed, u, coef, z, const, *halos).reshape(preserved_vector.shape)


def solution(mesh):
    finer = Mesh(mesh.devices.reshape(8, 2, 4, 2, 2), AXES)
    placed = (P(None, GX, GY, None), P(), P(), P(), P(GX, GY, None))
    return jax.shard_map(
        shards, mesh=finer, in_specs=placed, out_specs=P(None, GX, GY, None), check_vma=False
    )
```

```python
import jax
import jax.numpy as jnp
from jax import lax
from jax.experimental import pallas as pl
from jax.experimental.pallas import tpu as pltpu
from jax.sharding import Mesh
from jax.sharding import PartitionSpec as P


NS = 9
NVAR = 14
NEWTON = 2
EPSILON = 1e-06
COURANT = 0.8
LANES = 128
F32 = jnp.float32


def species_constants(table, gas, index, const):
    for i in range(NS):
        row = index[i]
        r = jnp.full((8, LANES), gas[row], F32)
        a = [r * jnp.full((8, LANES), table[k, row], F32) for k in range(6)]
        rest = [a[0] - r, a[1] * 0.5, a[2] * (1.0 / 3.0), a[3] * 0.25, a[4] * 0.2]
        for k, value in enumerate([r] + a + rest):
            const[12 * i + k] = value


def coefficients(u, rows):
    rho = u[0]
    for i in range(1, NS):
        rho = rho + u[i]
    inv = 1.0 / rho
    vel = [u[NS + j] * inv for j in range(3)]
    square = vel[0] * vel[0] + vel[1] * vel[1] + vel[2] * vel[2]
    target = u[NS + 3] - 0.5 * rho * square
    mix = [None] * 7
    for i in range(NS):
        for k in range(7):
            term = u[i] * rows[12 * i + k]
            mix[k] = term if mix[k] is None else mix[k] + term
    r0, a1, a2, a3, a4, a5, a6 = mix
    b1, b2, b3, b4, b5 = a1 - r0, a2 * 0.5, a3 * (1.0 / 3.0), a4 * 0.25, a5 * 0.2
    temp = jnp.ones_like(rho)
    for _ in range(NEWTON):
        energy = a6 + temp * (b1 + temp * (b2 + temp * (b3 + temp * (b4 + temp * b5))))
        slope = b1 + temp * (a2 + temp * (a3 + temp * (a4 + temp * a5)))
        temp = temp - (energy - target) / slope
    slope = b1 + temp * (a2 + temp * (a3 + temp * (a4 + temp * a5)))
    g = r0 / slope
    p = r0 * temp
    c = jnp.sqrt((1.0 + g) * p * inv)
    kinetic = 0.5 * g * square
    phi = []
    for i in range(NS):
        e = [rows[12 * i + 6 + k] for k in range(6)]
        energy = e[0] + temp * (e[1] + temp * (e[2] + temp * (e[3] + temp * (e[4] + temp * e[5]))))
        phi.append(rows[12 * i] * temp - g * energy + kinetic)
    return p, g, c, phi, vel


def halves(u, rows):
    p, g, c, phi, _ = coefficients(u, rows)
    return [0.5 * x for x in [p, g, c] + phi]


def fetch(pairs, sem):
    copies = [pltpu.make_async_copy(src, dst, sem.at[i]) for i, (src, dst) in enumerate(pairs)]
    for copy in copies:
        copy.start()
    return copies


def cell_kernel(table_h, gas_h, index_h, u_h, wide_ref, xs_ref, xe_ref, ys_ref, ye_ref,
                table, gas, index, rows, u_ref, sem):
    for copy in fetch([(table_h, table), (gas_h, gas), (index_h, index), (u_h, u_ref)], sem):
        copy.wait()
    species_constants(table, gas, index, rows)

    def body(i, fastest):
        at = pl.ds(pl.multiple_of(i * 8, 8), 8)
        u = [u_ref[k, at, :] for k in range(NVAR)]
        c, vel = coefficients(u, rows)[2::2]
        return tuple(jnp.maximum(f, jnp.abs(v) + c) for f, v in zip(fastest, vel))

    zero = jnp.zeros((8, LANES), F32)
    fastest = lax.fori_loop(0, 8, body, (zero, zero, zero), unroll=4)
    lane = lax.broadcasted_iota(jnp.int32, (8, LANES), 1)
    out = zero
    for d in range(3):
        top = jnp.max(jnp.max(fastest[d], axis=0, keepdims=True), axis=1, keepdims=True)
        out = jnp.where(lane == d, jnp.broadcast_to(top, (8, LANES)), out)
    for i in range(32):
        wide_ref[8 * i:8 * i + 8, :] = out
    for k in range(NVAR):
        xs_ref[k] = u_ref[k, 0:24, :]
        xe_ref[k] = u_ref[k, 40:64, :]
        for j in range(3):
            ys_ref[k, 8 * j:8 * j + 8, :] = u_ref[k, pl.ds(j, 8, stride=8), :]
            ye_ref[k, 8 * j:8 * j + 8, :] = u_ref[k, pl.ds(5 + j, 8, stride=8), :]


def correction(d0, d1, d2, d3):
    t0 = d0 - 1.375 * d1
    t1 = d1 - 0.625 * d2
    t2 = d3 - 1.375 * d2
    e1 = (0.609375 * d1) * d1 + 0.75 * EPSILON
    e2 = (0.609375 * d2) * d2 + 0.75 * EPSILON
    i0 = reciprocal(t0 * t0 + e1)
    i1 = reciprocal(t1 * t1 + e2)
    i2 = reciprocal(t2 * t2 + e2)
    w0 = i0 * i0
    w1 = i1 * i1
    w2 = 0.5 * (i2 * i2)
    q = 0.4375 * d2
    lead = (0.375 * d1 - q) - (1.0 / 3.0) * t0
    return q + (w0 * lead + w1 * t1 - w2 * t2) * reciprocal(w0 + 6.0 * (w1 + w2))


def reciprocal(x):
    return 1.0 / x


def split_fields(u, coef, order, speed):
    p, g, c, phi = coef[0], coef[1], coef[2], coef[3:]
    rho = u[0]
    for i in range(1, NS):
        rho = rho + u[i]
    inv = 0.5 / rho
    vel = [u[NS + j] * inv for j in order]
    plus, minus = vel[0] + speed, vel[0] - speed
    rows = u[:NS] + [u[NS + j] for j in order] + [u[NS + 3], u[NS + 4], rho]
    up = [x * plus for x in rows]
    down = [x * minus for x in rows]
    work = (p + p) * vel[0]
    for side in (up, down):
        side[NS] = side[NS] + p
        side[NS + 3] = side[NS + 3] + work
    mean = [x * inv for x in u[:NS]] + vel + [u[NS + 4] * inv, g, c] + phi
    return up, down, mean


def face_flux(left, right, jump, put):
    def mean(k):
        return left(k) + right(k)

    g, c = mean(13), mean(14)
    vel = [mean(9 + k) for k in range(3)]
    ig = 1.0 / g
    ic = 1.0 / c
    inv = ic * ic
    ihc = 0.5 * ic
    gs = g * inv
    gu = [gs * v for v in vel]
    square = vel[0] * vel[0] + vel[1] * vel[1] + vel[2] * vel[2]
    dot = None
    phis = []
    for k in range(NS):
        phi = mean(15 + k)
        term = mean(k) * phi
        dot = term if dot is None else dot + term
        phis.append(phi * inv)
    h = (c * c - dot) * ig + square
    pressure, swings, sums = {}, {}, {}
    for side in range(2):
        for i in range(side, 4 + side):
            dp = phis[0] * jump(side, i, 0)
            for k in range(1, NS):
                dp = dp + phis[k] * jump(side, i, k)
            v = [jump(side, i, NS + k) for k in range(3)]
            s = jump(side, i, 14)
            dp = dp + (gs * jump(side, i, 12) - (gu[0] * v[0] + gu[1] * v[1] + gu[2] * v[2]))
            pressure[side, i] = dp
            swings[side, i] = (v[0] - vel[0] * s) * ihc
            sums[side, i] = s

    def amplitude(wave):
        p = [wave(0, i) for i in range(4)]
        m = [wave(1, i) for i in range(4, 0, -1)]
        return correction(*p) - correction(*m)

    slower = amplitude(lambda side, i: 0.5 * pressure[side, i] - swings[side, i])
    faster = amplitude(lambda side, i: 0.5 * pressure[side, i] + swings[side, i])
    first = amplitude(lambda side, i: jump(side, i, 10) - vel[1] * sums[side, i])
    second = amplitude(lambda side, i: jump(side, i, 11) - vel[2] * sums[side, i])
    acoustic = slower + faster
    swing = (faster - slower) * c
    energy = h * acoustic + vel[0] * swing + vel[1] * first + vel[2] * second
    z = mean(12)
    put(13, z * acoustic + amplitude(lambda side, i: jump(side, i, 13) - z * pressure[side, i]))
    total = dot = None
    for k in range(NS):
        yk = mean(k)
        species = amplitude(lambda side, i: jump(side, i, k) - yk * pressure[side, i])
        put(k, yk * acoustic + species)
        term = phis[k] * species
        total = species if total is None else total + species
        dot = term if dot is None else dot + term
    both = acoustic + total
    put(9, vel[0] * both + swing)
    put(10, vel[1] * both + first)
    put(11, vel[2] * both + second)
    put(12, energy + square * total - (dot * (c * c)) * ig)


def own_kernel(table_h, gas_h, index_h, kind_h, u_ref, coef_ref, tall_ref, tall_coef, const_ref,
               table, gas, index, rows, kind, turned, sem):
    copies = fetch([(kind_h, kind), (table_h, table), (gas_h, gas), (index_h, index)], sem)
    copies[0].wait()
    sub = lax.broadcasted_iota(jnp.int32, (8, LANES), 0)
    lane = lax.broadcasted_iota(jnp.int32, (8, LANES), 1)
    left = lane < 64
    low_wall = kind[0, 0] == 1
    high_wall = kind[0, 1] == 1
    for pair in range(NVAR // 2):
        turned[pair] = jnp.concatenate([u_ref[2 * pair], u_ref[2 * pair + 1]], axis=0).T
    for k in range(NVAR):
        pair, second = divmod(k, 2)
        for b in range(8):
            top = turned[pair, pl.ds(b, 8, stride=8), :]
            bottom = turned[pair, pl.ds(64 + b, 8, stride=8), :]
            if second:
                tall_ref[k, b + 3] = jnp.where(left, pltpu.roll(top, 64, 1), bottom)
            else:
                tall_ref[k, b + 3] = jnp.where(left, top, pltpu.roll(bottom, 64, 1))
        sign = -1.0 if k == NS + 2 else 1.0
        for ghost in range(3):
            down = pltpu.roll(tall_ref[k, 10 - ghost], 1, 0)
            edge = jnp.where(low_wall, tall_ref[k, 3 + ghost] * sign, tall_ref[k, 3])
            edge = jnp.where(left, edge, pltpu.roll(down, 64, 1))
            tall_ref[k, 2 - ghost] = jnp.where(sub == 0, edge, down)
            up = pltpu.roll(tall_ref[k, 3 + ghost], 7, 0)
            edge = jnp.where(high_wall, tall_ref[k, 10 - ghost] * sign, tall_ref[k, 10])
            edge = jnp.where(left, pltpu.roll(up, 64, 1), edge)
            tall_ref[k, 11 + ghost] = jnp.where(sub == 7, edge, up)
    for copy in copies[1:]:
        copy.wait()
    species_constants(table, gas, index, rows)
    for k in range(12 * NS):
        const_ref[k] = rows[k, 0:1, :]

    def plane(i, _):
        at = pl.ds(pl.multiple_of(i * 8, 8), 8)
        for k, value in enumerate(halves([u_ref[k, at, :] for k in range(NVAR)], rows)):
            coef_ref[k, at, :] = value
        return 0

    lax.fori_loop(0, 8, plane, 0, unroll=4)

    def tall(i, _):
        for k, value in enumerate(halves([tall_ref[k, i] for k in range(NVAR)], rows)):
            tall_coef[k, i] = value
        return 0

    lax.fori_loop(0, 14, tall, 0, unroll=4 if 14 % 4 == 0 else 2)


def emit(flux, f, base):
    def put(k, value):
        flux[f, k] = value + base(k)

    return put


def column_kernel(wide, tall_ref, tall_coef, out_ref, speed_ref, pm, mean, jumps, fz, turned):
    top = wide[0:8, :]
    for i in range(1, 32):
        top = jnp.maximum(top, wide[8 * i:8 * i + 8, :])
    top = jnp.max(top, axis=0, keepdims=True)
    lane = lax.broadcasted_iota(jnp.int32, (1, LANES), 1)
    speeds = []
    for d in range(3):
        one = jnp.max(jnp.where(lane == d, top, 0.0), axis=1, keepdims=True)
        speeds.append(jnp.broadcast_to(0.5 * one, (8, LANES)))
    for d in range(3):
        speed_ref[d] = speeds[d]
    speed_ref[3] = (0.5 * COURANT) / (speeds[0] + speeds[1] + speeds[2])

    def cell(i, _):
        up, down, m = split_fields([tall_ref[k, i] for k in range(NVAR)],
                                   [tall_coef[k, i] for k in range(12)], (2, 0, 1), speeds[2])
        for k in range(24):
            mean[i, k] = m[k]
        for k in range(15):
            pm[i, k] = up[k]
            pm[i, 15 + k] = down[k]
        return 0

    lax.fori_loop(0, 14, cell, 0, unroll=2)

    def jump(i, _):
        for k in range(30):
            jumps[i, k] = pm[i + 1, k] - pm[i, k]
        return 0

    lax.fori_loop(0, 13, jump, 0, unroll=True)

    def face(f, _):
        face_flux(lambda k: mean[f + 2, k], lambda k: mean[f + 3, k],
                  lambda side, i, k: jumps[f + i, 15 * side + k],
                  emit(fz, f, lambda k: pm[f + 2, k] + pm[f + 3, 15 + k]))
        return 0

    lax.fori_loop(0, 9, face, 0)
    left = lax.broadcasted_iota(jnp.int32, (8, LANES), 1) < 64
    at_z = {9: 10, 10: 11, 11: 9}
    for pair in range(NVAR // 2):
        first, second = [at_z.get(k, k) for k in (2 * pair, 2 * pair + 1)]
        for b in range(8):
            x = fz[b, first] - fz[b + 1, first]
            y = fz[b, second] - fz[b + 1, second]
            turned[pair, pl.ds(b, 8, stride=8), :] = jnp.where(left, x, pltpu.roll(y, 64, 1))
            turned[pair, pl.ds(64 + b, 8, stride=8), :] = jnp.where(left, pltpu.roll(x, 64, 1), y)
    for pair in range(NVAR // 2):
        back = turned[pair].T
        out_ref[2 * pair] = back[0:64]
        out_ref[2 * pair + 1] = back[64:128]


def line_flux(order, strided, speed, u_ref, coef_ref, const, halos, pm, mean, jumps, flux, done):
    def cell(i, u, coef):
        up, down, m = split_fields(u, coef, order, speed)
        for k in range(24):
            mean[i, k] = m[k]
        for k in range(15):
            pm[i, k] = up[k]
            pm[i, 15 + k] = down[k]

    def own(i, _):
        at = pl.ds(i, 8, stride=8) if strided else pl.ds(pl.multiple_of(i * 8, 8), 8)
        cell(i + 3, [u_ref[k, at, :] for k in range(NVAR)],
             [coef_ref[k, at, :] for k in range(12)])
        return 0

    lax.fori_loop(0, 8, own, 0, unroll=2)
    for high in range(2):
        def halo(i, _, high=high):
            at = pl.ds(pl.multiple_of(i * 8, 8), 8)
            u = [halos[high][k, at, :] for k in range(NVAR)]
            cell(i + 11 * high, u, halves(u, const))
            return 0

        lax.fori_loop(0, 3, halo, 0, unroll=True)

    def jump(i, _):
        for k in range(30):
            jumps[i, k] = pm[i + 1, k] - pm[i, k]
        return 0

    lax.fori_loop(0, 13, jump, 0, unroll=True)

    def face(f, _):
        face_flux(lambda k: mean[f + 2, k], lambda k: mean[f + 3, k],
                  lambda side, i, k: jumps[f + i, 15 * side + k],
                  emit(flux, f, lambda k: pm[f + 2, k] + pm[f + 3, 15 + k]))
        pl.when(f > 0)(lambda: done(f - 1))
        return 0

    lax.fori_loop(0, 9, face, 0)


def x_kernel(speed_ref, u_ref, coef_ref, z_ref, const, low, high, out_ref, pm, mean, jumps, flux):
    def done(i):
        at = pl.ds(pl.multiple_of(i * 8, 8), 8)
        for k in range(NVAR):
            out_ref[k, at, :] = z_ref[k, at, :] + (flux[i, k] - flux[i + 1, k])

    line_flux((0, 1, 2), False, speed_ref[0], u_ref, coef_ref, const, (low, high), pm, mean, jumps,
              flux, done)


def y_kernel(speed_ref, u_ref, coef_ref, sum_ref, const, low, high, out_h,
             pm, mean, jumps, flux, out_ref, out_sem):
    scale = speed_ref[3]
    at_y = {9: 10, 10: 9, 11: 11}

    def done(j):
        at = pl.ds(j, 8, stride=8)
        for k in range(NVAR):
            ky = at_y.get(k, k)
            out_ref[k, at, :] = (sum_ref[k, at, :] + (flux[j, ky] - flux[j + 1, ky])) * scale

    line_flux((1, 0, 2), True, speed_ref[1], u_ref, coef_ref, const, (low, high), pm, mean, jumps,
              flux, done)
    copies = fetch([(out_ref.at[k], out_h.at[k]) for k in range(NVAR)], out_sem)
    for copy in copies:
        copy.wait()


HBM = pl.BlockSpec(memory_space=pltpu.MemorySpace.HBM)
VMEM = pl.BlockSpec(memory_space=pltpu.VMEM)
PLANES = (8, LANES)
TABLES = [pltpu.SMEM((6, 32), F32), pltpu.SMEM((32,), F32), pltpu.SMEM((NS,), jnp.int32),
          pltpu.VMEM((12 * NS,) + PLANES, F32)]


def struct(*shape):
    return jax.ShapeDtypeStruct(shape, F32)


def vmem(*shape):
    return pltpu.VMEM(shape, F32)


def dma(n):
    return pltpu.SemaphoreType.DMA((n,))


def params(mib=20):
    return pltpu.CompilerParams(vmem_limit_bytes=mib << 20)


def cells(table, gas, index, u):
    halo = struct(NVAR, 24, LANES)
    return pl.pallas_call(
        cell_kernel, name="cells", in_specs=[HBM] * 4, out_specs=[VMEM] * 5,
        out_shape=[struct(256, LANES), halo, halo, halo, halo],
        scratch_shapes=TABLES + [vmem(NVAR, 64, LANES), dma(4)],
        compiler_params=params())(*[
            pltpu.with_memory_space_constraint(x, pltpu.MemorySpace.HBM) for x in (table, gas, index, u)])


def own_cells(table, gas, index, kind, u):
    return pl.pallas_call(
        own_kernel, name="own_cells", in_specs=[HBM] * 4 + [VMEM], out_specs=[VMEM] * 4,
        out_shape=[struct(12, 64, LANES), struct(NVAR, 14, 8, LANES), struct(12, 14, 8, LANES),
                   struct(12 * NS, 1, LANES)],
        scratch_shapes=TABLES + [pltpu.SMEM((1, 2), jnp.int32),
                                     vmem(NVAR // 2, LANES, LANES), dma(4)],
        compiler_params=params())(table, gas, index, kind, u)


def columns(wide, tall, tall_coef):
    return pl.pallas_call(
        column_kernel, name="columns", in_specs=[VMEM] * 3, out_specs=[VMEM] * 2,
        out_shape=[struct(NVAR, 64, LANES), struct(4, 8, LANES)],
        scratch_shapes=[vmem(14, 30, *PLANES), vmem(14, 24, *PLANES), vmem(13, 30, *PLANES),
                        vmem(9, NVAR, *PLANES), vmem(NVAR // 2, LANES, LANES)],
        compiler_params=params())(wide, tall, tall_coef)


def x_rates(speed, u, coef, z, const, low, high):
    return pl.pallas_call(
        x_kernel, name="x_rates", in_specs=[VMEM] * 7, out_specs=VMEM,
        out_shape=struct(NVAR, 64, LANES),
        scratch_shapes=[vmem(14, 30, *PLANES), vmem(14, 24, *PLANES), vmem(13, 30, *PLANES),
                        vmem(9, NVAR, *PLANES)],
        compiler_params=params())(speed, u, coef, z, const, low, high)


def y_rates(speed, u, coef, total, const, low, high):
    return pl.pallas_call(
        y_kernel, name="y_rates", in_specs=[VMEM] * 7, out_specs=HBM,
        out_shape=struct(NVAR, 64, LANES),
        scratch_shapes=[vmem(14, 30, *PLANES), vmem(14, 24, *PLANES), vmem(13, 30, *PLANES),
                        vmem(9, NVAR, *PLANES), vmem(NVAR, 64, LANES), dma(NVAR)],
        compiler_params=params())(speed, u, coef, total, const, low, high)


AXES = ("z", "yl", "x", "yh", "c")
GX = ("z", "yl")
GY = ("x", "yh", "c")


def neighbours(start, end, axis):
    up = [(i, (i + 1) % 16) for i in range(16)]
    low = lax.ppermute(end, axis, up)
    high = lax.ppermute(start, axis, [(b, a) for a, b in up])
    return low, high


def shards(preserved_vector, nasa_table, gas_constant, species_index, face_kind):
    u = preserved_vector.reshape(NVAR, 64, LANES)
    fixed = (nasa_table.T, gas_constant, species_index)
    wide, xs, xe, ys, ye = cells(*fixed, u)
    wide = lax.all_to_all(wide, AXES, 0, 0, tiled=True)
    coef, tall, tall_coef, const = own_cells(*fixed, face_kind.reshape(1, 2), u)
    x_halos = neighbours(xs, xe, GX)
    y_halos = neighbours(ys, ye, GY)
    z, speed = columns(wide, tall, tall_coef)
    total = x_rates(speed, u, coef, z, const, *x_halos)
    return y_rates(speed, u, coef, total, const, *y_halos).reshape(preserved_vector.shape)


def solution(mesh):
    finer = Mesh(mesh.devices.reshape(8, 2, 4, 2, 2), AXES)
    placed = (P(None, GX, GY, None), P(), P(), P(), P(GX, GY, None))
    return jax.shard_map(
        shards, mesh=finer, in_specs=placed, out_specs=P(None, GX, GY, None), check_vma=False
    )
```

```python
import jax
import jax.numpy as jnp
from jax import lax
from jax.experimental import pallas as pl
from jax.experimental.pallas import tpu as pltpu
from jax.sharding import Mesh
from jax.sharding import PartitionSpec as P


NS = 9
NVAR = 14
NEWTON = 2
EPSILON = 1e-06
COURANT = 0.8
LANES = 128
F32 = jnp.float32


def species_constants(table, gas, index, const):
    for i in range(NS):
        row = index[i]
        r = jnp.full((8, LANES), gas[row], F32)
        a = [r * jnp.full((8, LANES), table[k, row], F32) for k in range(6)]
        rest = [a[0] - r, a[1] * 0.5, a[2] * (1.0 / 3.0), a[3] * 0.25, a[4] * 0.2]
        for k, value in enumerate([r] + a + rest):
            const[12 * i + k] = value


def coefficients(u, rows):
    rho = u[0]
    for i in range(1, NS):
        rho = rho + u[i]
    inv = 1.0 / rho
    vel = [u[NS + j] * inv for j in range(3)]
    square = vel[0] * vel[0] + vel[1] * vel[1] + vel[2] * vel[2]
    target = u[NS + 3] - 0.5 * rho * square
    mix = [None] * 7
    for i in range(NS):
        for k in range(7):
            term = u[i] * rows[12 * i + k]
            mix[k] = term if mix[k] is None else mix[k] + term
    r0, a1, a2, a3, a4, a5, a6 = mix
    b1, b2, b3, b4, b5 = a1 - r0, a2 * 0.5, a3 * (1.0 / 3.0), a4 * 0.25, a5 * 0.2
    temp = jnp.ones_like(rho)
    for _ in range(NEWTON):
        energy = a6 + temp * (b1 + temp * (b2 + temp * (b3 + temp * (b4 + temp * b5))))
        slope = b1 + temp * (a2 + temp * (a3 + temp * (a4 + temp * a5)))
        temp = temp - (energy - target) / slope
    slope = b1 + temp * (a2 + temp * (a3 + temp * (a4 + temp * a5)))
    g = r0 / slope
    p = r0 * temp
    c = jnp.sqrt((1.0 + g) * p * inv)
    kinetic = 0.5 * g * square
    phi = []
    for i in range(NS):
        e = [rows[12 * i + 6 + k] for k in range(6)]
        energy = e[0] + temp * (e[1] + temp * (e[2] + temp * (e[3] + temp * (e[4] + temp * e[5]))))
        phi.append(rows[12 * i] * temp - g * energy + kinetic)
    return p, g, c, phi, vel


def halves(u, rows):
    p, g, c, phi, _ = coefficients(u, rows)
    return [0.5 * x for x in [p, g, c] + phi]


def fetch(pairs, sem):
    copies = [pltpu.make_async_copy(src, dst, sem.at[i]) for i, (src, dst) in enumerate(pairs)]
    for copy in copies:
        copy.start()
    return copies


def cell_kernel(table_h, gas_h, index_h, u_h, wide_ref, xs_ref, xe_ref, ys_ref, ye_ref,
                table, gas, index, rows, u_ref, sem):
    for copy in fetch([(table_h, table), (gas_h, gas), (index_h, index), (u_h, u_ref)], sem):
        copy.wait()
    species_constants(table, gas, index, rows)

    def body(i, fastest):
        at = pl.ds(pl.multiple_of(i * 8, 8), 8)
        u = [u_ref[k, at, :] for k in range(NVAR)]
        c, vel = coefficients(u, rows)[2::2]
        return tuple(jnp.maximum(f, jnp.abs(v) + c) for f, v in zip(fastest, vel))

    zero = jnp.zeros((8, LANES), F32)
    fastest = lax.fori_loop(0, 8, body, (zero, zero, zero), unroll=4)
    lane = lax.broadcasted_iota(jnp.int32, (8, LANES), 1)
    out = zero
    for d in range(3):
        top = jnp.max(jnp.max(fastest[d], axis=0, keepdims=True), axis=1, keepdims=True)
        out = jnp.where(lane == d, jnp.broadcast_to(top, (8, LANES)), out)
    for i in range(32):
        wide_ref[8 * i:8 * i + 8, :] = out
    for k in range(NVAR):
        xs_ref[k] = u_ref[k, 0:24, :]
        xe_ref[k] = u_ref[k, 40:64, :]
        for j in range(3):
            ys_ref[k, 8 * j:8 * j + 8, :] = u_ref[k, pl.ds(j, 8, stride=8), :]
            ye_ref[k, 8 * j:8 * j + 8, :] = u_ref[k, pl.ds(5 + j, 8, stride=8), :]


def correction(d0, d1, d2, d3):
    t0 = d0 - 1.375 * d1
    t1 = d1 - 0.625 * d2
    t2 = d3 - 1.375 * d2
    e1 = (0.609375 * d1) * d1 + 0.75 * EPSILON
    e2 = (0.609375 * d2) * d2 + 0.75 * EPSILON
    i0 = reciprocal(t0 * t0 + e1)
    i1 = reciprocal(t1 * t1 + e2)
    i2 = reciprocal(t2 * t2 + e2)
    w0 = i0 * i0
    w1 = i1 * i1
    w2 = 0.5 * (i2 * i2)
    q = 0.4375 * d2
    lead = (0.375 * d1 - q) - (1.0 / 3.0) * t0
    return q + (w0 * lead + w1 * t1 - w2 * t2) * reciprocal(w0 + 6.0 * (w1 + w2))


def reciprocal(x):
    return 1.0 / x


def split_fields(u, coef, order, speed):
    p, g, c, phi = coef[0], coef[1], coef[2], coef[3:]
    rho = u[0]
    for i in range(1, NS):
        rho = rho + u[i]
    inv = 0.5 / rho
    vel = [u[NS + j] * inv for j in order]
    plus, minus = vel[0] + speed, vel[0] - speed
    rows = u[:NS] + [u[NS + j] for j in order] + [u[NS + 3], u[NS + 4], rho]
    up = [x * plus for x in rows]
    down = [x * minus for x in rows]
    work = (p + p) * vel[0]
    for side in (up, down):
        side[NS] = side[NS] + p
        side[NS + 3] = side[NS + 3] + work
    mean = [x * inv for x in u[:NS]] + vel + [u[NS + 4] * inv, g, c] + phi
    return up, down, mean


def face_flux(left, right, jump, put):
    def mean(k):
        return left(k) + right(k)

    g, c = mean(13), mean(14)
    vel = [mean(9 + k) for k in range(3)]
    ig = 1.0 / g
    ic = 1.0 / c
    inv = ic * ic
    ihc = 0.5 * ic
    gs = g * inv
    gu = [gs * v for v in vel]
    square = vel[0] * vel[0] + vel[1] * vel[1] + vel[2] * vel[2]
    dot = None
    phis = []
    for k in range(NS):
        phi = mean(15 + k)
        term = mean(k) * phi
        dot = term if dot is None else dot + term
        phis.append(phi * inv)
    h = (c * c - dot) * ig + square
    pressure, swings, sums = {}, {}, {}
    for side in range(2):
        for i in range(side, 4 + side):
            dp = phis[0] * jump(side, i, 0)
            for k in range(1, NS):
                dp = dp + phis[k] * jump(side, i, k)
            v = [jump(side, i, NS + k) for k in range(3)]
            s = jump(side, i, 14)
            dp = dp + (gs * jump(side, i, 12) - (gu[0] * v[0] + gu[1] * v[1] + gu[2] * v[2]))
            pressure[side, i] = dp
            swings[side, i] = (v[0] - vel[0] * s) * ihc
            sums[side, i] = s

    def amplitude(wave):
        p = [wave(0, i) for i in range(4)]
        m = [wave(1, i) for i in range(4, 0, -1)]
        return correction(*p) - correction(*m)

    slower = amplitude(lambda side, i: 0.5 * pressure[side, i] - swings[side, i])
    faster = amplitude(lambda side, i: 0.5 * pressure[side, i] + swings[side, i])
    first = amplitude(lambda side, i: jump(side, i, 10) - vel[1] * sums[side, i])
    second = amplitude(lambda side, i: jump(side, i, 11) - vel[2] * sums[side, i])
    acoustic = slower + faster
    swing = (faster - slower) * c
    energy = h * acoustic + vel[0] * swing + vel[1] * first + vel[2] * second
    z = mean(12)
    put(13, z * acoustic + amplitude(lambda side, i: jump(side, i, 13) - z * pressure[side, i]))
    total = dot = None
    for k in range(NS):
        yk = mean(k)
        species = amplitude(lambda side, i: jump(side, i, k) - yk * pressure[side, i])
        put(k, yk * acoustic + species)
        term = phis[k] * species
        total = species if total is None else total + species
        dot = term if dot is None else dot + term
    both = acoustic + total
    put(9, vel[0] * both + swing)
    put(10, vel[1] * both + first)
    put(11, vel[2] * both + second)
    put(12, energy + square * total - (dot * (c * c)) * ig)


def own_kernel(table_h, gas_h, index_h, kind_h, u_ref, coef_ref, tall_ref, tall_coef, const_ref,
               table, gas, index, rows, kind, turned, sem):
    copies = fetch([(kind_h, kind), (table_h, table), (gas_h, gas), (index_h, index)], sem)
    copies[0].wait()
    sub = lax.broadcasted_iota(jnp.int32, (8, LANES), 0)
    lane = lax.broadcasted_iota(jnp.int32, (8, LANES), 1)
    left = lane < 64
    low_wall = kind[0, 0] == 1
    high_wall = kind[0, 1] == 1
    for pair in range(NVAR // 2):
        turned[pair] = jnp.concatenate([u_ref[2 * pair], u_ref[2 * pair + 1]], axis=0).T
    for k in range(NVAR):
        pair, second = divmod(k, 2)
        for b in range(8):
            top = turned[pair, pl.ds(b, 8, stride=8), :]
            bottom = turned[pair, pl.ds(64 + b, 8, stride=8), :]
            if second:
                tall_ref[k, b + 3] = jnp.where(left, pltpu.roll(top, 64, 1), bottom)
            else:
                tall_ref[k, b + 3] = jnp.where(left, top, pltpu.roll(bottom, 64, 1))
        sign = -1.0 if k == NS + 2 else 1.0
        for ghost in range(3):
            down = pltpu.roll(tall_ref[k, 10 - ghost], 1, 0)
            edge = jnp.where(low_wall, tall_ref[k, 3 + ghost] * sign, tall_ref[k, 3])
            edge = jnp.where(left, edge, pltpu.roll(down, 64, 1))
            tall_ref[k, 2 - ghost] = jnp.where(sub == 0, edge, down)
            up = pltpu.roll(tall_ref[k, 3 + ghost], 7, 0)
            edge = jnp.where(high_wall, tall_ref[k, 10 - ghost] * sign, tall_ref[k, 10])
            edge = jnp.where(left, pltpu.roll(up, 64, 1), edge)
            tall_ref[k, 11 + ghost] = jnp.where(sub == 7, edge, up)
    for copy in copies[1:]:
        copy.wait()
    species_constants(table, gas, index, rows)
    for k in range(12 * NS):
        const_ref[k] = rows[k, 0:1, :]

    def plane(i, _):
        at = pl.ds(pl.multiple_of(i * 8, 8), 8)
        for k, value in enumerate(halves([u_ref[k, at, :] for k in range(NVAR)], rows)):
            coef_ref[k, at, :] = value
        return 0

    lax.fori_loop(0, 8, plane, 0, unroll=4)

    def tall(i, _):
        for k, value in enumerate(halves([tall_ref[k, i] for k in range(NVAR)], rows)):
            tall_coef[k, i] = value
        return 0

    lax.fori_loop(0, 14, tall, 0, unroll=4 if 14 % 4 == 0 else 2)


def emit(flux, f, base):
    def put(k, value):
        flux[f, k] = value + base(k)

    return put


def column_kernel(wide, tall_ref, tall_coef, out_ref, speed_ref, pm, mean, jumps, fz, turned):
    top = wide[0:8, :]
    for i in range(1, 32):
        top = jnp.maximum(top, wide[8 * i:8 * i + 8, :])
    top = jnp.max(top, axis=0, keepdims=True)
    lane = lax.broadcasted_iota(jnp.int32, (1, LANES), 1)
    speeds = []
    for d in range(3):
        one = jnp.max(jnp.where(lane == d, top, 0.0), axis=1, keepdims=True)
        speeds.append(jnp.broadcast_to(0.5 * one, (8, LANES)))
    for d in range(3):
        speed_ref[d] = speeds[d]
    speed_ref[3] = (0.5 * COURANT) / (speeds[0] + speeds[1] + speeds[2])

    def cell(i, _):
        up, down, m = split_fields([tall_ref[k, i] for k in range(NVAR)],
                                   [tall_coef[k, i] for k in range(12)], (2, 0, 1), speeds[2])
        for k in range(24):
            mean[i, k] = m[k]
        for k in range(15):
            pm[i, k] = up[k]
            pm[i, 15 + k] = down[k]
        return 0

    lax.fori_loop(0, 14, cell, 0, unroll=7)

    def jump(i, _):
        for k in range(30):
            jumps[i, k] = pm[i + 1, k] - pm[i, k]
        return 0

    lax.fori_loop(0, 13, jump, 0, unroll=True)

    def face(f, _):
        face_flux(lambda k: mean[f + 2, k], lambda k: mean[f + 3, k],
                  lambda side, i, k: jumps[f + i, 15 * side + k],
                  emit(fz, f, lambda k: pm[f + 2, k] + pm[f + 3, 15 + k]))
        return 0

    lax.fori_loop(0, 9, face, 0)
    left = lax.broadcasted_iota(jnp.int32, (8, LANES), 1) < 64
    at_z = {9: 10, 10: 11, 11: 9}
    for pair in range(NVAR // 2):
        first, second = [at_z.get(k, k) for k in (2 * pair, 2 * pair + 1)]
        for b in range(8):
            x = fz[b, first] - fz[b + 1, first]
            y = fz[b, second] - fz[b + 1, second]
            turned[pair, pl.ds(b, 8, stride=8), :] = jnp.where(left, x, pltpu.roll(y, 64, 1))
            turned[pair, pl.ds(64 + b, 8, stride=8), :] = jnp.where(left, pltpu.roll(x, 64, 1), y)
    for pair in range(NVAR // 2):
        back = turned[pair].T
        out_ref[2 * pair] = back[0:64]
        out_ref[2 * pair + 1] = back[64:128]


def line_flux(order, strided, speed, u_ref, coef_ref, const, halos, pm, mean, jumps, flux, done):
    def cell(i, u, coef):
        up, down, m = split_fields(u, coef, order, speed)
        for k in range(24):
            mean[i, k] = m[k]
        for k in range(15):
            pm[i, k] = up[k]
            pm[i, 15 + k] = down[k]

    def own(i, _):
        at = pl.ds(i, 8, stride=8) if strided else pl.ds(pl.multiple_of(i * 8, 8), 8)
        cell(i + 3, [u_ref[k, at, :] for k in range(NVAR)],
             [coef_ref[k, at, :] for k in range(12)])
        return 0

    lax.fori_loop(0, 8, own, 0, unroll=8)
    for high in range(2):
        def halo(i, _, high=high):
            at = pl.ds(pl.multiple_of(i * 8, 8), 8)
            u = [halos[high][k, at, :] for k in range(NVAR)]
            cell(i + 11 * high, u, halves(u, const))
            return 0

        lax.fori_loop(0, 3, halo, 0, unroll=True)

    def jump(i, _):
        for k in range(30):
            jumps[i, k] = pm[i + 1, k] - pm[i, k]
        return 0

    lax.fori_loop(0, 13, jump, 0, unroll=True)

    def face(f, _):
        face_flux(lambda k: mean[f + 2, k], lambda k: mean[f + 3, k],
                  lambda side, i, k: jumps[f + i, 15 * side + k],
                  emit(flux, f, lambda k: pm[f + 2, k] + pm[f + 3, 15 + k]))
        pl.when(f > 0)(lambda: done(f - 1))
        return 0

    lax.fori_loop(0, 9, face, 0)


def x_kernel(speed_ref, u_ref, coef_ref, z_ref, const, low, high, out_ref, pm, mean, jumps, flux):
    def done(i):
        at = pl.ds(pl.multiple_of(i * 8, 8), 8)
        for k in range(NVAR):
            out_ref[k, at, :] = z_ref[k, at, :] + (flux[i, k] - flux[i + 1, k])

    line_flux((0, 1, 2), False, speed_ref[0], u_ref, coef_ref, const, (low, high), pm, mean, jumps,
              flux, done)


def y_kernel(speed_ref, u_ref, coef_ref, sum_ref, const, low, high, out_h,
             pm, mean, jumps, flux, out_ref, out_sem):
    scale = speed_ref[3]
    at_y = {9: 10, 10: 9, 11: 11}

    def done(j):
        at = pl.ds(j, 8, stride=8)
        for k in range(NVAR):
            ky = at_y.get(k, k)
            out_ref[k, at, :] = (sum_ref[k, at, :] + (flux[j, ky] - flux[j + 1, ky])) * scale

    line_flux((1, 0, 2), True, speed_ref[1], u_ref, coef_ref, const, (low, high), pm, mean, jumps,
              flux, done)
    copies = fetch([(out_ref.at[pl.ds(k, 7)], out_h.at[pl.ds(k, 7)]) for k in (0, 7)], out_sem)
    for copy in copies:
        copy.wait()


HBM = pl.BlockSpec(memory_space=pltpu.MemorySpace.HBM)
VMEM = pl.BlockSpec(memory_space=pltpu.VMEM)
PLANES = (8, LANES)
TABLES = [pltpu.SMEM((6, 32), F32), pltpu.SMEM((32,), F32), pltpu.SMEM((NS,), jnp.int32),
          pltpu.VMEM((12 * NS,) + PLANES, F32)]


def struct(*shape):
    return jax.ShapeDtypeStruct(shape, F32)


def vmem(*shape):
    return pltpu.VMEM(shape, F32)


def dma(n):
    return pltpu.SemaphoreType.DMA((n,))


def params(mib=20):
    return pltpu.CompilerParams(vmem_limit_bytes=mib << 20)


def cells(table, gas, index, u):
    halo = struct(NVAR, 24, LANES)
    return pl.pallas_call(
        cell_kernel, name="cells", in_specs=[HBM] * 4, out_specs=[VMEM] * 5,
        out_shape=[struct(256, LANES), halo, halo, halo, halo],
        scratch_shapes=TABLES + [vmem(NVAR, 64, LANES), dma(4)],
        compiler_params=params())(*[
            pltpu.with_memory_space_constraint(x, pltpu.MemorySpace.HBM) for x in (table, gas, index, u)])


def own_cells(table, gas, index, kind, u):
    return pl.pallas_call(
        own_kernel, name="own_cells", in_specs=[HBM] * 4 + [VMEM], out_specs=[VMEM] * 4,
        out_shape=[struct(12, 64, LANES), struct(NVAR, 14, 8, LANES), struct(12, 14, 8, LANES),
                   struct(12 * NS, 1, LANES)],
        scratch_shapes=TABLES + [pltpu.SMEM((1, 2), jnp.int32),
                                     vmem(NVAR // 2, LANES, LANES), dma(4)],
        compiler_params=params())(table, gas, index, kind, u)


def columns(wide, tall, tall_coef):
    return pl.pallas_call(
        column_kernel, name="columns", in_specs=[VMEM] * 3, out_specs=[VMEM] * 2,
        out_shape=[struct(NVAR, 64, LANES), struct(4, 8, LANES)],
        scratch_shapes=[vmem(14, 30, *PLANES), vmem(14, 24, *PLANES), vmem(13, 30, *PLANES),
                        vmem(9, NVAR, *PLANES), vmem(NVAR // 2, LANES, LANES)],
        compiler_params=params())(wide, tall, tall_coef)


def x_rates(speed, u, coef, z, const, low, high):
    return pl.pallas_call(
        x_kernel, name="x_rates", in_specs=[VMEM] * 7, out_specs=VMEM,
        out_shape=struct(NVAR, 64, LANES),
        scratch_shapes=[vmem(14, 30, *PLANES), vmem(14, 24, *PLANES), vmem(13, 30, *PLANES),
                        vmem(9, NVAR, *PLANES)],
        compiler_params=params())(speed, u, coef, z, const, low, high)


def y_rates(speed, u, coef, total, const, low, high):
    return pl.pallas_call(
        y_kernel, name="y_rates", in_specs=[VMEM] * 7, out_specs=HBM,
        out_shape=struct(NVAR, 64, LANES),
        scratch_shapes=[vmem(14, 30, *PLANES), vmem(14, 24, *PLANES), vmem(13, 30, *PLANES),
                        vmem(9, NVAR, *PLANES), vmem(NVAR, 64, LANES), dma(2)],
        compiler_params=params())(speed, u, coef, total, const, low, high)


AXES = ("z", "yl", "x", "yh", "c")
GX = ("z", "yl")
GY = ("x", "yh", "c")


def neighbours(start, end, axis):
    up = [(i, (i + 1) % 16) for i in range(16)]
    low = lax.ppermute(end, axis, up)
    high = lax.ppermute(start, axis, [(b, a) for a, b in up])
    return low, high


def shards(preserved_vector, nasa_table, gas_constant, species_index, face_kind):
    u = preserved_vector.reshape(NVAR, 64, LANES)
    fixed = (nasa_table.T, gas_constant, species_index)
    wide, xs, xe, ys, ye = cells(*fixed, u)
    wide = lax.all_to_all(wide, AXES, 0, 0, tiled=True)
    coef, tall, tall_coef, const = own_cells(*fixed, face_kind.reshape(1, 2), u)
    x_halos = neighbours(xs, xe, GX)
    y_halos = neighbours(ys, ye, GY)
    z, speed = columns(wide, tall, tall_coef)
    total = x_rates(speed, u, coef, z, const, *x_halos)
    return y_rates(speed, u, coef, total, const, *y_halos).reshape(preserved_vector.shape)


def solution(mesh):
    finer = Mesh(mesh.devices.reshape(8, 2, 4, 2, 2), AXES)
    placed = (P(None, GX, GY, None), P(), P(), P(), P(GX, GY, None))
    return jax.shard_map(
        shards, mesh=finer, in_specs=placed, out_specs=P(None, GX, GY, None), check_vma=False
    )
```
